32 devices in a mesh: ctx: 4 (over z), exp: 8 (over y, x, core).
Axes of the slice: x: 2, y: 2, z: 4, core: 2. Of those that a mesh axis runs over, the one named last changes fastest.
Arguments:
- seq_inputs: bfloat16 [2048, 2048], P('ctx', 'exp'), may hold values from -6 to 6
- step_size: float32 [32, 2048], P('exp', 'ctx'), may hold values from 0.0007 to 0.14
- write_map: bfloat16 [16, 2048], P(None, 'ctx'), may hold values from -2 to 2
- read_map: bfloat16 [16, 2048], P(None, 'ctx'), may hold values from -2 to 2
- decay_log: float32 [32], P('exp'), may hold values from -9.3 to 1.4
- skip_gain: float32 [32], P('exp'), may hold values from 0.5 to 1.5
- moe_tokens: bfloat16 [1024, 4096], P('exp'), may hold values from -6 to 6
- expert_ids: int32 [1024, 2], P('exp'), may hold values from 0 to 3, all different within a row; in each aligned block of 128 rows (0 to 127, 128 to 255, ...) at most 128 rows name the same one
- route_weights: float32 [1024, 2], P('exp'), may hold values from 0.1 to 1
- gate_proj: bfloat16 [8, 4096, 3584], P('exp', None, 'ctx'), may hold values from -0.09375 to 0.09375
- up_proj: bfloat16 [8, 4096, 3584], P('exp', None, 'ctx'), may hold values from -0.09375 to 0.09375
- down_proj: bfloat16 [8, 3584, 4096], P('exp', None, 'ctx'), may hold values from -0.0625 to 0.0625
Outputs:
- mixer_output: bfloat16 [2048, 2048], P('ctx', 'exp')
- expert_output: bfloat16 [1024, 4096], P('exp', 'ctx')
The draws below stay inside these ranges and needn't reach their ends.
Inputs may be any that keep to these rules, and one draw needn't show every extreme that they name: `expert_ids`: each row names two different experts. In the 128 rows of one index of exp (aligned blocks), no expert is named more than 128 times, and in some blocks an expert is named exactly 128 times.
All inputs are finite; a program needn't handle non-finite values.
Results may differ from the reference program's by a relative error of at most 0.002.
The reference program's roundings to bfloat16 on the way count: a program that leaves them out, or rounds other values in their place, can miss the bound.
Values may be sent and summed in bfloat16 or wider, within the bound.
A program may use at most 64 MiB of HBM per device.

```python
import math
import jax
import jax.numpy as jnp
import numpy as np
from jax import lax

D = 4096
FF = 7168
EXPERTS = 4
MOE_DEV = 128
MOE_TOKENS = 1024
CAP = 128
HEADS = 32
HEAD_SIZE = 64
STATE = 16
BLOCK = 256
SEQ = 2048
N_EXP = 8


def draw_step_size(key, part):
    first, second = jax.random.split(key)
    base = jax.random.uniform(first, (HEADS, SEQ), jnp.float32, math.log(0.002), math.log(0.05))
    region = jax.random.uniform(second, (HEADS, SEQ // BLOCK), jnp.float32, -1.0, 1.0)
    return jnp.exp(base + jnp.repeat(region, BLOCK, axis=1)).astype(jnp.float32)


def draw_decay_log(key, part):
    first, second, third = jax.random.split(key, 3)
    share = 0.5
    keeping = jax.random.bernoulli(first, share, (HEADS,))
    slower = jax.random.uniform(second, (HEADS,), jnp.float32, math.log(0.0001), math.log(0.0004))
    faster = jax.random.uniform(third, (HEADS,), jnp.float32, 0.0, math.log(4.0))
    return jnp.where(keeping, slower, faster).astype(jnp.float32)


def block_levels(key, shape, cuts, least, high):
    gain, own = 1.0, jax.random.fold_in(key, 6)
    for position, parts in cuts:
        draws = jnp.exp(jax.random.uniform(jax.random.fold_in(own, position), (parts,), jnp.float32, least / len(cuts), high / len(cuts)))
        gain = gain * jnp.repeat(draws, shape[position] // parts).reshape([-1 if axis == position else 1 for axis in range(len(shape))])
    return gain


def deal_out(rng, own, number, rows, count, top, bound, lean):
    ranking = jax.random.permutation(rng, count)
    crowded, ordinary = shares(count, rows * top, bound, lean, True), shares(count, rows * top, bound, lean, False)
    places = jnp.arange(count)

    def named(tallies, turn):
        used = int((tallies > 0).sum())
        fixed = max(1, used // 4)
        shifted = fixed + (places - fixed + turn * (used - fixed)) % max(1, count - fixed)
        return jnp.zeros((count,), jnp.int32).at[ranking[jnp.where(places < fixed, places, shifted)]].set(jnp.asarray(tallies, jnp.int32))

    tallies = jnp.where(number % 4 == 0, named(crowded, number // 4), named(ordinary, number - number // 4 - 1))
    mixed = jax.random.permutation(jax.random.fold_in(own, 3), count)
    source_of, sink = mixed[0:count // 2 * 2:2], mixed[1:count // 2 * 2:2]
    room = jnp.minimum(tallies[source_of] - 1, bound - tallies[sink]) // 2
    room = jnp.where((source_of == ranking[0]) | (sink == ranking[0]) | (tallies[sink] == 0), 0, jnp.maximum(room, 0))
    shifted = jax.random.randint(jax.random.fold_in(own, 4), (count // 2,), 0, 1 << 20) % (room + 1)
    tallies = tallies.at[source_of].add(-shifted).at[sink].add(shifted)
    labels = jnp.searchsorted(jnp.cumsum(tallies), jnp.arange(rows * top), side="right").astype(jnp.int32)
    table = labels.reshape(top, rows).T
    table = table[jax.random.permutation(jax.random.fold_in(own, 1), rows)]
    turn = jax.random.randint(jax.random.fold_in(own, 2), (rows, 1), 0, top)
    return jnp.take_along_axis(table, (jnp.arange(top)[None, :] + turn) % top, axis=1)


def shares(number_of, total, most, slope, full):
    weights = [(1 << 20) // math.isqrt(grade ** slope) + 1 for grade in range(1, number_of + 1)]
    largest = most if full else min(most, max(-(-total // number_of), total * weights[0] // sum(weights)))
    least = 1 if total - largest >= number_of - 1 else 0
    counts, surplus = [largest] + [least] * (number_of - 1), total - largest - least * (number_of - 1)
    while surplus > 0:
        movable = [i for i in range(1, number_of) if counts[i] < largest] or [i for i in range(1, number_of) if counts[i] < most]
        mass, remaining = sum([weights[i] for i in movable]), surplus
        for i in movable:
            extra = min(most - counts[i], max(1, remaining * weights[i] // mass), surplus)
            counts[i] = counts[i] + extra
            surplus = surplus - extra
    return np.array(counts)


def bell_draw(key, extent, width, reach, cuts=(), kind=jnp.bfloat16):
    array = jax.random.normal(key, extent, jnp.float32) * width
    if len(cuts) > 0:
        array = block_levels(key, extent, cuts, -0.22, 0.18) * array
    return jnp.clip(array, min=-reach, max=reach).astype(kind)


def setup_inputs(seed: int = 0) -> dict:
    key_list = jax.random.split(jax.random.key(seed), 13)
    seq_inputs = bell_draw(key_list[0], (SEQ, HEADS * HEAD_SIZE), 1.0, 6.0, ((0, 4), (1, 8)))
    step_size = draw_step_size(jax.random.fold_in(key_list[12], 71), 0)
    write_map = bell_draw(key_list[2], (STATE, SEQ), 0.3, 2.0, ((1, 4),))
    read_map = bell_draw(key_list[3], (STATE, SEQ), 0.3, 2.0, ((1, 4),))
    decay_log = draw_decay_log(jax.random.fold_in(key_list[12], 71), 0)
    skip_gain = jnp.clip(0.5 + 1.0 * jax.random.uniform(key_list[5], (HEADS,), jnp.float32) ** block_levels(key_list[5], (HEADS,), ((0, 8),), -0.2, 0.2), 0.5, 1.5)
    moe_tokens = bell_draw(key_list[6], (MOE_TOKENS, D), 1.0, 6.0, ((0, 8),))
    expert_ids_keys = jax.random.split(jax.random.fold_in(key_list[7], 1), MOE_TOKENS // MOE_DEV)
    expert_ids_turns = jax.random.permutation(jax.random.fold_in(key_list[7], 3), MOE_TOKENS // MOE_DEV)
    expert_ids = jax.vmap(lambda own, number: deal_out(jax.random.fold_in(key_list[7], 2), own, number, MOE_DEV, EXPERTS, 2, CAP, 2))(expert_ids_keys, expert_ids_turns).reshape((MOE_TOKENS, 2))
    route_weights = jnp.clip(0.1 + 0.9 * jax.random.uniform(key_list[8], (MOE_TOKENS, 2), jnp.float32) ** block_levels(key_list[8], (MOE_TOKENS, 2), ((0, 8),), -0.2, 0.2), 0.1, 1.0)
    gate_proj = bell_draw(key_list[9], (2 * EXPERTS, D, FF // 2), D ** -0.5, 0.09375, ((0, 8), (2, 4)))
    up_proj = bell_draw(key_list[10], (2 * EXPERTS, D, FF // 2), D ** -0.5, 0.09375, ((0, 8), (2, 4)))
    down_proj = bell_draw(key_list[11], (2 * EXPERTS, FF // 2, D), FF ** -0.5, 0.0625, ((0, 8), (2, 4)))
    return dict(seq_inputs=seq_inputs, step_size=step_size, write_map=write_map, read_map=read_map, decay_log=decay_log, skip_gain=skip_gain, moe_tokens=moe_tokens, expert_ids=expert_ids, route_weights=route_weights, gate_proj=gate_proj, up_proj=up_proj, down_proj=down_proj)


HIGHEST = lax.Precision.HIGHEST


def mixer_reference(seq_inputs, step_size, write_map, read_map, decay_log, skip_gain):
    length = seq_inputs.shape[0]
    head_count = step_size.shape[0]
    state_count = write_map.shape[0]
    head_width = seq_inputs.shape[1] // head_count
    block_count = length // BLOCK
    decay_rate = -jnp.exp(decay_log)
    log_decay = (step_size * decay_rate[:, None]).reshape(head_count, block_count, BLOCK).transpose(1, 0, 2)
    step_blocks = step_size.reshape(head_count, block_count, BLOCK).transpose(1, 0, 2)
    write_blocks = write_map.reshape(state_count, block_count, BLOCK).transpose(1, 0, 2)
    read_blocks = read_map.reshape(state_count, block_count, BLOCK).transpose(1, 0, 2)
    value_blocks = seq_inputs.reshape(block_count, BLOCK, head_count, head_width)
    row_index = lax.broadcasted_iota(jnp.int32, (BLOCK, BLOCK), 0)
    column_index = lax.broadcasted_iota(jnp.int32, (BLOCK, BLOCK), 1)
    lower = column_index <= row_index

    def one_block(running, pieces):
        log_part, step_part, write_part, read_part, value_part = pieces
        cumulative = jnp.cumsum(log_part, axis=1)
        block_end = cumulative[:, BLOCK - 1]
        scores = jnp.dot(read_part.T, write_part, preferred_element_type=jnp.float32)
        difference = cumulative[:, :, None] - cumulative[:, None, :]
        decay = jnp.where(lower[None], jnp.exp(jnp.minimum(difference, 0.0)), 0.0)
        mixing = (scores[None] * decay * step_part[:, None, :]).astype(jnp.bfloat16)
        values = value_part.astype(jnp.float32)
        local_mix = jnp.einsum("hts,shp->thp", mixing.astype(jnp.float32), values)
        carried = jnp.einsum("nt,hnp->thp", read_part.astype(jnp.float32), running, precision=HIGHEST)
        carried = carried * jnp.exp(cumulative).T[:, :, None]
        output = local_mix + carried + skip_gain[None, :, None] * values
        weights = jnp.exp(block_end[:, None] - cumulative) * step_part
        key_decayed = (write_part[None] * weights[:, None, :]).astype(jnp.bfloat16)
        increment = jnp.einsum("hns,shp->hnp", key_decayed.astype(jnp.float32), values)
        running = jnp.exp(block_end)[:, None, None] * running + increment
        return running, output.astype(jnp.bfloat16)

    zero_state = jnp.zeros((head_count, state_count, head_width), jnp.float32)
    final_state, outputs = lax.scan(one_block, zero_state, (log_decay, step_blocks, write_blocks, read_blocks, value_blocks))
    return outputs.reshape(length, head_count * head_width)


def expert_reference(moe_tokens, expert_ids, route_weights, gate_proj, up_proj, down_proj):
    total_tokens = moe_tokens.shape[0]
    model_width = moe_tokens.shape[1]
    group_size = total_tokens // N_EXP
    expert_count = gate_proj.shape[0] // 2
    assigned = expert_ids.reshape(N_EXP, group_size * 2)
    onehot = (assigned[:, :, None] == jnp.arange(expert_count, dtype=jnp.int32)[None, None, :]).astype(jnp.int32)
    earlier_count = jnp.cumsum(onehot, axis=1) - onehot
    slot_index = jnp.sum(earlier_count * onehot, axis=2).astype(jnp.int32)
    group_index = jnp.broadcast_to(jnp.arange(N_EXP, dtype=jnp.int32)[:, None], assigned.shape)
    token_index = group_index * group_size + jnp.arange(group_size * 2, dtype=jnp.int32)[None, :] // 2
    table = jnp.full((expert_count, N_EXP, CAP), total_tokens, jnp.int32)
    table = table.at[assigned, group_index, slot_index].set(token_index.astype(jnp.int32))
    padded = jnp.concatenate([moe_tokens, jnp.zeros((1, model_width), jnp.bfloat16)], axis=0)

    def run_expert(expert):
        rows_in = padded[table[expert].reshape(-1)]
        gate_full = jnp.concatenate([gate_proj[2 * expert], gate_proj[2 * expert + 1]], axis=1)
        up_full = jnp.concatenate([up_proj[2 * expert], up_proj[2 * expert + 1]], axis=1)
        down_full = jnp.concatenate([down_proj[2 * expert], down_proj[2 * expert + 1]], axis=0)
        gate_sums = jnp.dot(rows_in, gate_full, preferred_element_type=jnp.float32)
        up_sums = jnp.dot(rows_in, up_full, preferred_element_type=jnp.float32)
        hidden = (jax.nn.silu(gate_sums) * up_sums).astype(jnp.bfloat16)
        return jnp.dot(hidden, down_full, preferred_element_type=jnp.float32)

    results = lax.map(run_expert, jnp.arange(expert_count, dtype=jnp.int32))
    results = results.reshape(expert_count, N_EXP, CAP, model_width)
    picked = results[assigned, group_index, slot_index]
    weighted = picked * route_weights.reshape(N_EXP, group_size * 2)[:, :, None]
    mixed = jnp.sum(weighted.reshape(total_tokens, 2, model_width), axis=1)
    return mixed.astype(jnp.bfloat16)


def reference(seq_inputs, step_size, write_map, read_map, decay_log, skip_gain, moe_tokens, expert_ids, route_weights, gate_proj, up_proj, down_proj):
    return (mixer_reference(seq_inputs, step_size, write_map, read_map, decay_log, skip_gain),
            expert_reference(moe_tokens, expert_ids, route_weights, gate_proj, up_proj, down_proj))
```

```python
import functools

import jax
import jax.numpy as jnp
from jax import lax
from jax.experimental import pallas as pl
from jax.experimental.pallas import tpu as pltpu
from jax.sharding import PartitionSpec as P

BLOCK = 256


HIGHEST = lax.Precision.HIGHEST


def carried_in(part, axis, combine, identity):
    place = lax.axis_index(axis)
    gathered = jax.tree.map(lambda a: lax.all_gather(a, axis), part)
    state = jax.tree.map(lambda a, e: jnp.zeros_like(a) + jnp.asarray(e, a.dtype), part, identity)

    def one(lap, state):
        return combine(
            state, jax.tree.map(lambda a: lax.dynamic_index_in_dim(a, lap, 0, False), gathered)
        )

    return lax.fori_loop(0, place, one, state)


def combine_states(former, latter):
    return (former[0] + latter[0], jnp.exp(latter[0])[:, None, None] * former[1] + latter[1])


def block_chain(running, pieces):
    decay, increment = pieces
    return (decay[:, None, None] * running + increment, running)


def mixer_prepare(seq_inputs, step_size, write_map, read_map, decay_log):
    length = seq_inputs.shape[0]
    head_count = step_size.shape[0]
    state_count = write_map.shape[0]
    head_width = seq_inputs.shape[1] // head_count
    block_count = length // BLOCK
    decay_rate = -jnp.exp(decay_log)
    log_decay = (step_size * decay_rate[:, None]).reshape(head_count, block_count, BLOCK)
    cumulative = jnp.cumsum(log_decay, axis=2)
    block_ends = cumulative[:, :, BLOCK - 1]
    step_blocks = step_size.reshape(head_count, block_count, BLOCK)
    write_blocks = write_map.reshape(state_count, block_count, BLOCK)
    read_blocks = read_map.reshape(state_count, block_count, BLOCK)
    value_blocks = seq_inputs.reshape(block_count, BLOCK, head_count, head_width)
    scores = jnp.einsum(
        "nkt,nks->kts", read_blocks, write_blocks, preferred_element_type=jnp.float32
    )
    row_index = lax.broadcasted_iota(jnp.int32, (BLOCK, BLOCK), 0)
    column_index = lax.broadcasted_iota(jnp.int32, (BLOCK, BLOCK), 1)
    lower = column_index <= row_index
    difference = cumulative[:, :, :, None] - cumulative[:, :, None, :]
    decay = jnp.where(lower[None, None], jnp.exp(jnp.minimum(difference, 0.0)), 0.0)
    mixing = (scores[None] * decay * step_blocks[:, :, None, :]).astype(jnp.bfloat16)
    local_mix = jnp.einsum(
        "hkts,kshp->kthp", mixing, value_blocks, preferred_element_type=jnp.float32
    )
    weights = jnp.exp(block_ends[:, :, None] - cumulative) * step_blocks
    key_decayed = (write_blocks[None] * weights[:, None]).astype(jnp.bfloat16)
    increments = jnp.einsum(
        "hnks,kshp->khnp", key_decayed, value_blocks, preferred_element_type=jnp.float32
    )
    zero_state = jnp.zeros((head_count, state_count, head_width), jnp.float32)
    final, entering = lax.scan(block_chain, zero_state, (jnp.exp(block_ends).T, increments))
    return (local_mix, cumulative, block_ends, entering, final)


def mixer_finish(
    local_mix, cumulative, block_ends, entering, state_before, read_map, seq_inputs, skip_gain
):
    head_count = block_ends.shape[0]
    block_count = block_ends.shape[1]
    state_count = read_map.shape[0]
    head_width = entering.shape[3]
    before = jnp.cumsum(block_ends, axis=1) - block_ends
    states = jnp.exp(before).T[:, :, None, None] * state_before[None] + entering
    read_blocks = read_map.reshape(state_count, block_count, BLOCK).astype(jnp.float32)
    carried = jnp.einsum("nkt,khnp->kthp", read_blocks, states, precision=HIGHEST)
    carried = carried * jnp.exp(cumulative).transpose(1, 2, 0)[:, :, :, None]
    value_blocks = seq_inputs.reshape(block_count, BLOCK, head_count, head_width).astype(
        jnp.float32
    )
    output = local_mix + carried + skip_gain[None, None, :, None] * value_blocks
    return output.reshape(seq_inputs.shape).astype(jnp.bfloat16)


def expert_block(moe_tokens, expert_ids, route_weights, gate_proj, up_proj, down_proj):
    group_size = moe_tokens.shape[0]
    model_width = moe_tokens.shape[1]
    expert_count = lax.axis_size("exp") // 2
    capacity = min(group_size, 4 * group_size // expert_count)
    slot_count = expert_count * capacity
    assigned = expert_ids.reshape(group_size * 2)
    onehot = (
        assigned[:, None] == lax.broadcasted_iota(jnp.int32, (group_size * 2, expert_count), 1)
    ).astype(jnp.int32)
    earlier_count = jnp.cumsum(onehot, axis=0) - onehot
    position = jnp.sum((earlier_count + assigned[:, None] * capacity) * onehot, axis=1)
    matches = (
        position[:, None] == lax.broadcasted_iota(jnp.int32, (group_size * 2, slot_count), 1)
    ).astype(jnp.float32)
    dispatch = jnp.sum(matches.reshape(group_size, 2, slot_count), axis=1).astype(jnp.bfloat16)
    combine = jnp.sum(
        (matches * route_weights.reshape(group_size * 2)[:, None]).reshape(
            group_size, 2, slot_count
        ),
        axis=1,
    )
    gate_weight = gate_proj[0]
    up_weight = up_proj[0]
    down_weight = down_proj[0]
    packed = jnp.einsum(
        "is,id->sd", dispatch, moe_tokens, preferred_element_type=jnp.float32
    ).astype(jnp.bfloat16)
    doubled = jnp.broadcast_to(
        packed.reshape(expert_count, 1, capacity, model_width),
        (expert_count, 2, capacity, model_width),
    )
    arrived = lax.all_to_all(
        doubled.reshape(2 * slot_count, model_width), "exp", split_axis=0, concat_axis=0, tiled=True
    )
    gate_sums = jnp.dot(arrived, gate_weight, preferred_element_type=jnp.float32)
    up_sums = jnp.dot(arrived, up_weight, preferred_element_type=jnp.float32)
    hidden = (jax.nn.silu(gate_sums) * up_sums).astype(jnp.bfloat16)
    partial_out = jnp.dot(
        lax.all_gather(hidden, "ctx", axis=1, tiled=True),
        down_weight,
        preferred_element_type=jnp.float32,
    )
    returned = lax.all_to_all(partial_out, "exp", split_axis=0, concat_axis=0, tiled=True)
    summed = jnp.sum(returned.reshape(expert_count, 2, capacity, -1), axis=1).reshape(
        slot_count, -1
    )
    result = jnp.dot(combine, summed, precision=HIGHEST, preferred_element_type=jnp.float32)
    return result.astype(jnp.bfloat16)


MESH = pl.DeviceIdType.MESH
VMEM_BYTES = 60 * 2**20
GRID = 2
PAIR = 2


def expert_kernel(
    lines,
    tok_in,
    share,
    gate_hbm,
    up_hbm,
    down_hbm,
    out,
    gate_w,
    up_w,
    down_w,
    tok,
    hid,
    acc,
    swap,
    res,
    ret,
    load_sem,
    tsend,
    trecv,
    hsend_r,
    hsend_l,
    hrecv_l,
    hrecv_r,
    xsend,
    xrecv,
    rsend,
    rrecv,
):
    chunks = GRID * GRID
    z = lax.axis_index("ctx")
    e = lax.axis_index("exp")
    half = lax.rem(e, PAIR)
    other = 1 - half
    px = lax.rem(e // PAIR, GRID)
    py = e // (PAIR * GRID)
    rows = tok_in.shape[0]
    sub = rows // 2

    def peer(c, core):
        qx = lax.rem(px + lax.rem(c, GRID), GRID)
        qy = lax.rem(py + c // GRID, GRID)
        return (z, (qy * GRID + qx) * PAIR + core)

    mine = pl.ds(pl.multiple_of(half * rows, rows), rows)
    theirs = pl.ds(pl.multiple_of(other * rows, rows), rows)
    partner = (z, (py * GRID + px) * PAIR + other)

    loads = [
        pltpu.make_async_copy(gate_hbm, gate_w, load_sem.at[0]),
        pltpu.make_async_copy(up_hbm, up_w, load_sem.at[1]),
        pltpu.make_async_copy(tok_in, tok.at[0, mine], load_sem.at[3]),
        pltpu.make_async_copy(down_hbm, down_w, load_sem.at[2]),
    ]
    for load in loads:
        load.start()

    barrier = pltpu.get_barrier_semaphore()
    for device in (partner, peer(1, half), peer(2, half), peer(3, half)):
        pl.semaphore_signal(barrier, inc=1, device_id=device, device_id_type=MESH)

    @pl.when(z > 0)
    def _():
        pl.semaphore_signal(barrier, inc=1, device_id=(z - 1, e), device_id_type=MESH)

    @pl.when(z < lines - 1)
    def _():
        pl.semaphore_signal(barrier, inc=1, device_id=(z + 1, e), device_id_type=MESH)

    neighbours = 4 + jnp.where(z > 0, 1, 0) + jnp.where(z < lines - 1, 1, 0)
    pl.semaphore_wait(barrier, neighbours)

    def remote(src, dst, ssem, rsem, device):
        return pltpu.make_async_remote_copy(
            src_ref=src,
            dst_ref=dst,
            send_sem=ssem,
            recv_sem=rsem,
            device_id=device,
            device_id_type=MESH,
        )

    upper = pl.ds(pl.multiple_of(half * rows, rows), sub)
    lower = pl.ds(pl.multiple_of(half * rows + sub, sub), sub)
    copies = [
        remote(tok_in, tok.at[0, mine], tsend.at[0], trecv.at[0], partner),
        remote(tok_in, tok.at[1, mine], tsend.at[1], trecv.at[1], peer(1, half)),
        remote(tok_in, tok.at[2, mine], tsend.at[2], trecv.at[2], peer(2, half)),
        remote(
            tok.at[1, upper], tok.at[3, upper], tsend.at[3], trecv.at[3], peer(2, half)
        ),
        remote(
            tok.at[2, lower], tok.at[3, lower], tsend.at[4], trecv.at[4], peer(1, half)
        ),
        remote(tok.at[1, mine], tok.at[1, mine], tsend.at[5], trecv.at[5], partner),
        remote(tok.at[2, mine], tok.at[2, mine], tsend.at[6], trecv.at[6], partner),
        remote(tok.at[3, mine], tok.at[3, mine], tsend.at[7], trecv.at[7], partner),
    ]
    for copy in copies[:3]:
        copy.start()

    def make_hidden(c):
        width = gate_w.shape[1]
        x = tok[c]
        g = jnp.dot(x, gate_w[...], preferred_element_type=jnp.float32)
        u = jnp.dot(x, up_w[...], preferred_element_type=jnp.float32)
        hid[z, c] = (jax.nn.silu(g) * u).astype(jnp.bfloat16)

    def to_right(d, c):
        j = z - d
        return remote(hid.at[j, c], hid.at[j, c], hsend_r.at[d, c], hrecv_l.at[d, c], (z + 1, e))

    def to_left(d, c):
        j = z + d
        return remote(hid.at[j, c], hid.at[j, c], hsend_l.at[d, c], hrecv_r.at[d, c], (z - 1, e))

    def from_left(d, c):
        return remote(
            hid.at[z - d, c], hid.at[z - d, c], hsend_r.at[d, c], hrecv_l.at[d - 1, c], (z - 1, e)
        )

    def from_right(d, c):
        return remote(
            hid.at[z + d, c], hid.at[z + d, c], hsend_l.at[d, c], hrecv_r.at[d - 1, c], (z + 1, e)
        )

    def send_own(c):
        @pl.when(z < lines - 1)
        def _():
            to_right(0, c).start()

        @pl.when(z > 0)
        def _():
            to_left(0, c).start()

    def pass_on(d, c):
        @pl.when(z >= d)
        def _():
            from_left(d, c).wait_recv()

            @pl.when(z < lines - 1)
            def _():
                to_right(d, c).start()

        @pl.when(z + d < lines)
        def _():
            from_right(d, c).wait_recv()

            @pl.when(z > 0)
            def _():
                to_left(d, c).start()

    def add_down(j, c):
        acc[c] += jnp.dot(hid[j, c], down_w[j], preferred_element_type=jnp.float32)

    def add_both(d, c):
        @pl.when(z >= d)
        def _():
            add_down(z - d, c)

        @pl.when(z + d < lines)
        def _():
            add_down(z + d, c)

    loads[2].wait()
    loads[0].wait()
    loads[1].wait()
    copies[0].wait_recv()
    make_hidden(0)
    send_own(0)
    loads[3].wait()

    def chunk(c, carry):
        acc[c] = jnp.dot(hid[z, c], down_w[z], preferred_element_type=jnp.float32)
        pass_on(1, c)

        @pl.when(c == 0)
        def _():
            copies[1].wait_recv()
            copies[5].start()
            copies[3].start()
            copies[2].wait_recv()
            copies[6].start()
            copies[4].start()
            copies[5].wait_recv()

        @pl.when(c == 1)
        def _():
            copies[3].wait_recv()
            copies[4].wait_recv()
            copies[7].start()
            copies[6].wait_recv()

        @pl.when(c == 2)
        def _():
            copies[7].wait_recv()

        @pl.when(c < chunks - 1)
        def _():
            make_hidden(c + 1)

        for d in range(2, lines):
            pass_on(d, c)
            if d == 2:

                @pl.when(c < chunks - 1)
                def _():
                    send_own(c + 1)

            add_both(d - 1, c)
        add_both(lines - 1, c)

        exchange = remote(acc.at[c, theirs], swap.at[c], xsend.at[c], xrecv.at[c], partner)
        exchange.start()
        exchange.wait_recv()
        res[c] = acc[c, mine] + swap[c]

        @pl.when(c > 0)
        def _():
            remote(res.at[c], ret.at[c], rsend.at[c], rrecv.at[c], peer(c, half)).start()

        return carry

    lax.fori_loop(0, chunks, chunk, 0)

    total = share[:, 0:1] * res[0]
    for c in range(1, chunks):
        remote(res.at[c], ret.at[c], rsend.at[c], rrecv.at[c], peer(c, half)).wait_recv()
        total += share[:, c : c + 1] * ret[c]
    out[...] = total.astype(out.dtype)

    for copy in copies:
        copy.wait_send()
    for c in range(chunks):
        for d in range(lines - 1):

            @pl.when((z >= d) & (z < lines - 1))
            def _():
                to_right(d, c).wait_send()

            @pl.when((z + d < lines) & (z > 0))
            def _():
                to_left(d, c).wait_send()

        remote(acc.at[c, theirs], swap.at[c], xsend.at[c], xrecv.at[c], partner).wait_send()
        if c > 0:
            remote(res.at[c], ret.at[c], rsend.at[c], rrecv.at[c], peer(c, half)).wait_send()


def expert_fused(moe_tokens, expert_ids, route_weights, gate_proj, up_proj, down_proj):
    lines = lax.axis_size("ctx")
    chunks = GRID * GRID
    rows, width = moe_tokens.shape
    part = gate_proj.shape[2]
    columns = down_proj.shape[2]
    place = lax.axis_index("exp") // PAIR
    px, py = place % GRID, place // GRID
    order = jnp.stack(
        [((py + c // GRID) % GRID) * GRID + (px + c % GRID) % GRID for c in range(chunks)]
    )
    share = jnp.sum(
        jnp.where(expert_ids[:, :, None] == order[None, None, :], route_weights[:, :, None], 0.0),
        axis=1,
    )
    f32, bf16 = jnp.float32, jnp.bfloat16
    dma = pltpu.SemaphoreType.DMA
    vmem = pl.BlockSpec(memory_space=pltpu.VMEM)
    hbm = pl.BlockSpec(memory_space=pl.ANY)
    return pl.pallas_call(
        functools.partial(expert_kernel, lines),
        out_shape=jax.ShapeDtypeStruct((rows, columns), bf16),
        in_specs=[vmem, vmem, hbm, hbm, hbm],
        out_specs=vmem,
        scratch_shapes=[
            pltpu.VMEM((width, part), bf16),
            pltpu.VMEM((width, part), bf16),
            pltpu.VMEM((lines, part, columns), bf16),
            pltpu.VMEM((chunks, PAIR * rows, width), bf16),
            pltpu.VMEM((lines, chunks, PAIR * rows, part), bf16),
            pltpu.VMEM((chunks, PAIR * rows, columns), f32),
            pltpu.VMEM((chunks, rows, columns), f32),
            pltpu.VMEM((chunks, rows, columns), f32),
            pltpu.VMEM((chunks, rows, columns), f32),
            dma((4,)),
            dma((8,)),
            dma((8,)),
            dma((lines, chunks)),
            dma((lines, chunks)),
            dma((lines, chunks)),
            dma((lines, chunks)),
            dma((chunks,)),
            dma((chunks,)),
            dma((chunks,)),
            dma((chunks,)),
        ],
        compiler_params=pltpu.CompilerParams(
            collective_id=0, has_side_effects=True, vmem_limit_bytes=VMEM_BYTES
        ),
    )(
        moe_tokens,
        share,
        gate_proj[0],
        up_proj[0],
        down_proj[0].reshape(lines, part, columns),
    )


def expert_layer(*arrays):
    moe_tokens, gate_proj, down_proj = arrays[0], arrays[3], arrays[5]
    if lax.axis_size("exp") == PAIR * GRID * GRID and gate_proj.shape[2] % 128 == 0:
        return expert_fused(*arrays)
    return expert_block(*arrays)


def on_device(
    seq_inputs,
    step_size,
    write_map,
    read_map,
    decay_log,
    skip_gain,
    moe_tokens,
    expert_ids,
    route_weights,
    gate_proj,
    up_proj,
    down_proj,
):
    local_mix, cumulative, block_ends, entering, final = mixer_prepare(
        seq_inputs, step_size, write_map, read_map, decay_log
    )
    total_log = jnp.sum(block_ends, axis=1)
    log_before, state_before = carried_in(
        (total_log, final),
        "ctx",
        combine_states,
        (jnp.zeros_like(total_log), jnp.zeros_like(final)),
    )
    expert_output = expert_layer(
        moe_tokens, expert_ids, route_weights, gate_proj, up_proj, down_proj
    )
    mixer_output = mixer_finish(
        local_mix, cumulative, block_ends, entering, state_before, read_map, seq_inputs, skip_gain
    )
    return (mixer_output, expert_output)


def solution(mesh):
    return jax.shard_map(
        on_device,
        mesh=mesh,
        in_specs=(
            P("ctx", "exp"),
            P("exp", "ctx"),
            P(None, "ctx"),
            P(None, "ctx"),
            P("exp"),
            P("exp"),
            P("exp", None),
            P("exp", None),
            P("exp", None),
            P("exp", None, "ctx"),
            P("exp", None, "ctx"),
            P("exp", None, "ctx"),
        ),
        out_specs=(P("ctx", "exp"), P("exp", "ctx")),
        check_vma=False,
    )
```

```python
import functools

import jax
import jax.numpy as jnp
from jax import lax
from jax.experimental import pallas as pl
from jax.experimental.pallas import tpu as pltpu
from jax.sharding import PartitionSpec as P

BLOCK = 256


HIGHEST = lax.Precision.HIGHEST


def block_chain(running, pieces):
    decay, increment = pieces
    return (decay[:, None, None] * running + increment, running)


def mixer_prepare(seq_inputs, step_size, write_map, read_map, decay_log):
    length = seq_inputs.shape[0]
    head_count = step_size.shape[0]
    state_count = write_map.shape[0]
    head_width = seq_inputs.shape[1] // head_count
    block_count = length // BLOCK
    decay_rate = -jnp.exp(decay_log)
    log_decay = (step_size * decay_rate[:, None]).reshape(head_count, block_count, BLOCK)
    cumulative = jnp.cumsum(log_decay, axis=2)
    block_ends = cumulative[:, :, BLOCK - 1]
    step_blocks = step_size.reshape(head_count, block_count, BLOCK)
    write_blocks = write_map.reshape(state_count, block_count, BLOCK)
    read_blocks = read_map.reshape(state_count, block_count, BLOCK)
    value_blocks = seq_inputs.reshape(block_count, BLOCK, head_count, head_width)
    scores = jnp.einsum(
        "nkt,nks->kts", read_blocks, write_blocks, preferred_element_type=jnp.float32
    )
    row_index = lax.broadcasted_iota(jnp.int32, (BLOCK, BLOCK), 0)
    column_index = lax.broadcasted_iota(jnp.int32, (BLOCK, BLOCK), 1)
    lower = column_index <= row_index
    difference = cumulative[:, :, :, None] - cumulative[:, :, None, :]
    decay = jnp.where(lower[None, None], jnp.exp(jnp.minimum(difference, 0.0)), 0.0)
    mixing = (scores[None] * decay * step_blocks[:, :, None, :]).astype(jnp.bfloat16)
    local_mix = jnp.einsum(
        "hkts,kshp->kthp", mixing, value_blocks, preferred_element_type=jnp.float32
    )
    weights = jnp.exp(block_ends[:, :, None] - cumulative) * step_blocks
    key_decayed = (write_blocks[None] * weights[:, None]).astype(jnp.bfloat16)
    increments = jnp.einsum(
        "hnks,kshp->khnp", key_decayed, value_blocks, preferred_element_type=jnp.float32
    )
    zero_state = jnp.zeros((head_count, state_count, head_width), jnp.float32)
    final, entering = lax.scan(block_chain, zero_state, (jnp.exp(block_ends).T, increments))
    return (local_mix, cumulative, block_ends, entering, final)


def mixer_finish(
    local_mix, cumulative, block_ends, entering, state_before, read_map, seq_inputs, skip_gain
):
    head_count = block_ends.shape[0]
    block_count = block_ends.shape[1]
    state_count = read_map.shape[0]
    head_width = entering.shape[3]
    before = jnp.cumsum(block_ends, axis=1) - block_ends
    states = jnp.exp(before).T[:, :, None, None] * state_before[None] + entering
    read_blocks = read_map.reshape(state_count, block_count, BLOCK).astype(jnp.float32)
    carried = jnp.einsum("nkt,khnp->kthp", read_blocks, states, precision=HIGHEST)
    carried = carried * jnp.exp(cumulative).transpose(1, 2, 0)[:, :, :, None]
    value_blocks = seq_inputs.reshape(block_count, BLOCK, head_count, head_width).astype(
        jnp.float32
    )
    output = local_mix + carried + skip_gain[None, None, :, None] * value_blocks
    return output.reshape(seq_inputs.shape).astype(jnp.bfloat16)


def expert_block(moe_tokens, expert_ids, route_weights, gate_proj, up_proj, down_proj):
    group_size = moe_tokens.shape[0]
    model_width = moe_tokens.shape[1]
    expert_count = lax.axis_size("exp") // 2
    capacity = min(group_size, 4 * group_size // expert_count)
    slot_count = expert_count * capacity
    assigned = expert_ids.reshape(group_size * 2)
    onehot = (
        assigned[:, None] == lax.broadcasted_iota(jnp.int32, (group_size * 2, expert_count), 1)
    ).astype(jnp.int32)
    earlier_count = jnp.cumsum(onehot, axis=0) - onehot
    position = jnp.sum((earlier_count + assigned[:, None] * capacity) * onehot, axis=1)
    matches = (
        position[:, None] == lax.broadcasted_iota(jnp.int32, (group_size * 2, slot_count), 1)
    ).astype(jnp.float32)
    dispatch = jnp.sum(matches.reshape(group_size, 2, slot_count), axis=1).astype(jnp.bfloat16)
    combine = jnp.sum(
        (matches * route_weights.reshape(group_size * 2)[:, None]).reshape(
            group_size, 2, slot_count
        ),
        axis=1,
    )
    gate_weight = gate_proj[0]
    up_weight = up_proj[0]
    down_weight = down_proj[0]
    packed = jnp.einsum(
        "is,id->sd", dispatch, moe_tokens, preferred_element_type=jnp.float32
    ).astype(jnp.bfloat16)
    doubled = jnp.broadcast_to(
        packed.reshape(expert_count, 1, capacity, model_width),
        (expert_count, 2, capacity, model_width),
    )
    arrived = lax.all_to_all(
        doubled.reshape(2 * slot_count, model_width), "exp", split_axis=0, concat_axis=0, tiled=True
    )
    gate_sums = jnp.dot(arrived, gate_weight, preferred_element_type=jnp.float32)
    up_sums = jnp.dot(arrived, up_weight, preferred_element_type=jnp.float32)
    hidden = (jax.nn.silu(gate_sums) * up_sums).astype(jnp.bfloat16)
    partial_out = jnp.dot(
        lax.all_gather(hidden, "ctx", axis=1, tiled=True),
        down_weight,
        preferred_element_type=jnp.float32,
    )
    returned = lax.all_to_all(partial_out, "exp", split_axis=0, concat_axis=0, tiled=True)
    summed = jnp.sum(returned.reshape(expert_count, 2, capacity, -1), axis=1).reshape(
        slot_count, -1
    )
    result = jnp.dot(combine, summed, precision=HIGHEST, preferred_element_type=jnp.float32)
    return result.astype(jnp.bfloat16)


MESH = pl.DeviceIdType.MESH
VMEM_BYTES = 60 * 2**20
GRID = 2
PAIR = 2


def expert_kernel(
    lines,
    tok_in,
    share,
    packed,
    gate_hbm,
    up_hbm,
    down_hbm,
    out,
    gathered,
    gate_w,
    up_w,
    down_w,
    tok,
    hid,
    acc,
    swap,
    ret,
    far_w,
    acc2,
    swap2,
    ret2,
    edge_in,
    states,
    load_sem,
    tsend,
    trecv,
    hsend_r,
    hsend_l,
    hrecv_l,
    hrecv_r,
    xsend,
    xrecv,
    rsend,
    rrecv,
    ssend,
    srecv,
    wsend,
    wrecv,
    x2send,
    x2recv,
    r2send,
    r2recv,
    esend,
    erecv,
):
    chunks = GRID * GRID
    z = lax.axis_index("ctx")
    e = lax.axis_index("exp")
    half = lax.rem(e, PAIR)
    other = 1 - half
    px = lax.rem(e // PAIR, GRID)
    py = e // (PAIR * GRID)
    rows = tok_in.shape[0]
    sub = rows // 2

    def peer(c, core):
        qx = lax.rem(px + lax.rem(c, GRID), GRID)
        qy = lax.rem(py + c // GRID, GRID)
        return (z, (qy * GRID + qx) * PAIR + core)

    mine = pl.ds(pl.multiple_of(half * rows, rows), rows)
    theirs = pl.ds(pl.multiple_of(other * rows, rows), rows)
    partner = (z, (py * GRID + px) * PAIR + other)

    loads = [
        pltpu.make_async_copy(gate_hbm, gate_w, load_sem.at[0]),
        pltpu.make_async_copy(up_hbm, up_w, load_sem.at[1]),
        pltpu.make_async_copy(tok_in, tok.at[0, mine], load_sem.at[3]),
        pltpu.make_async_copy(down_hbm, down_w, load_sem.at[2]),
    ]
    for load in loads:
        load.start()

    barrier = pltpu.get_barrier_semaphore()
    for device in (partner, peer(1, half), peer(2, half), peer(3, half)):
        pl.semaphore_signal(barrier, inc=1, device_id=device, device_id_type=MESH)

    for j in range(lines):

        @pl.when(z != j)
        def _():
            pl.semaphore_signal(barrier, inc=1, device_id=(j, e), device_id_type=MESH)

    pl.semaphore_wait(barrier, 4 + lines - 1)

    def remote(src, dst, ssem, rsem, device):
        return pltpu.make_async_remote_copy(
            src_ref=src,
            dst_ref=dst,
            send_sem=ssem,
            recv_sem=rsem,
            device_id=device,
            device_id_type=MESH,
        )

    upper = pl.ds(pl.multiple_of(half * rows, rows), sub)
    lower = pl.ds(pl.multiple_of(half * rows + sub, sub), sub)
    copies = [
        remote(tok_in, tok.at[0, mine], tsend.at[0], trecv.at[0], partner),
        remote(tok_in, tok.at[1, mine], tsend.at[1], trecv.at[1], peer(1, half)),
        remote(tok_in, tok.at[2, mine], tsend.at[2], trecv.at[2], peer(2, half)),
        remote(
            tok.at[1, upper], tok.at[3, upper], tsend.at[3], trecv.at[3], peer(2, half)
        ),
        remote(
            tok.at[2, lower], tok.at[3, lower], tsend.at[4], trecv.at[4], peer(1, half)
        ),
        remote(tok.at[1, mine], tok.at[1, mine], tsend.at[5], trecv.at[5], partner),
        remote(tok.at[2, mine], tok.at[2, mine], tsend.at[6], trecv.at[6], partner),
        remote(tok.at[3, mine], tok.at[3, mine], tsend.at[7], trecv.at[7], partner),
    ]
    for copy in copies[:3]:
        copy.start()

    last = chunks - 1
    assist = lines > 3
    edge = (z == 0) | (z == lines - 1)
    helper = (z == 1) | (z == lines - 2)
    far = jnp.where(z < 2, lines - 1, 0)
    piece = far_w.shape[0] // chunks

    def lend(k):
        span = pl.ds(k * piece, piece)
        target = jnp.where(z == 0, 1, lines - 2)
        return remote(
            down_hbm.at[far, span], far_w.at[span], wsend.at[k], wrecv.at[k], (target, e)
        )

    def start_lend(k):
        if assist:

            @pl.when(edge)
            def _():
                lend(k).start()

    def state_copy(j):
        return remote(packed, states.at[z], ssend.at[j], srecv.at[z], (j, e))

    start_lend(0)
    for j in range(lines):

        @pl.when(z != j)
        def _():
            state_copy(j).start()

    states[z] = packed[...]

    def make_hidden(c):
        width = gate_w.shape[1]
        x = tok[c]
        g = jnp.dot(x, gate_w[...], preferred_element_type=jnp.float32)
        u = jnp.dot(x, up_w[...], preferred_element_type=jnp.float32)
        hid[z, c] = (jax.nn.silu(g) * u).astype(jnp.bfloat16)

    def to_right(d, c):
        j = z - d
        return remote(hid.at[j, c], hid.at[j, c], hsend_r.at[d, c], hrecv_l.at[d, c], (z + 1, e))

    def to_left(d, c):
        j = z + d
        return remote(hid.at[j, c], hid.at[j, c], hsend_l.at[d, c], hrecv_r.at[d, c], (z - 1, e))

    def from_left(d, c):
        return remote(
            hid.at[z - d, c], hid.at[z - d, c], hsend_r.at[d, c], hrecv_l.at[d - 1, c], (z - 1, e)
        )

    def from_right(d, c):
        return remote(
            hid.at[z + d, c], hid.at[z + d, c], hsend_l.at[d, c], hrecv_r.at[d - 1, c], (z + 1, e)
        )

    def send_own(c):
        @pl.when(z < lines - 1)
        def _():
            to_right(0, c).start()

        @pl.when(z > 0)
        def _():
            to_left(0, c).start()

    def needed(d, c):
        return (c == last) if assist and d == lines - 1 else True

    def pass_on(d, c):
        @pl.when((z >= d) & needed(d, c))
        def _():
            from_left(d, c).wait_recv()

            @pl.when((z < lines - 1) & needed(d + 1, c))
            def _():
                to_right(d, c).start()

        @pl.when((z + d < lines) & needed(d, c))
        def _():
            from_right(d, c).wait_recv()

            @pl.when((z > 0) & needed(d + 1, c))
            def _():
                to_left(d, c).start()

    def add_down(j, c):
        acc[c] += jnp.dot(hid[j, c], down_w[j], preferred_element_type=jnp.float32)

    def add_both(d, c):
        @pl.when((z >= d) & needed(d, c))
        def _():
            add_down(z - d, c)

        @pl.when((z + d < lines) & needed(d, c))
        def _():
            add_down(z + d, c)

    def exchange(total, landing, ssem, rsem, c):
        return remote(total.at[c, theirs], landing.at[c], ssem.at[c], rsem.at[c], partner)

    def bring_home(total, landing, ssem, rsem, c):
        return remote(total.at[c, mine], landing.at[c], ssem.at[c], rsem.at[c], peer(c, half))

    def end_copy():
        target = jnp.where(z == 1, 0, lines - 1)
        return remote(acc2.at[0, mine], edge_in, esend.at[0], erecv.at[0], (target, e))

    loads[2].wait()
    loads[0].wait()
    loads[1].wait()
    copies[0].wait_recv()
    make_hidden(0)
    send_own(0)
    start_lend(1)
    loads[3].wait()

    def chunk(c, carry):
        acc[c] = jnp.dot(hid[z, c], down_w[z], preferred_element_type=jnp.float32)
        pass_on(1, c)

        @pl.when(c == 0)
        def _():
            copies[1].wait_recv()
            copies[5].start()
            copies[3].start()
            copies[2].wait_recv()
            copies[6].start()
            copies[4].start()
            copies[5].wait_recv()

        @pl.when(c == 1)
        def _():
            copies[3].wait_recv()
            copies[4].wait_recv()
            copies[7].start()
            copies[6].wait_recv()

        @pl.when(c == 2)
        def _():
            copies[7].wait_recv()

        @pl.when(c < chunks - 1)
        def _():
            make_hidden(c + 1)

        if assist:

            @pl.when(helper & (c == last))
            def _():
                for k in range(chunks):
                    lend(k).wait_recv()
                for k in range(last):
                    acc2[k] = jnp.dot(
                        hid[far, k], far_w[...], preferred_element_type=jnp.float32
                    )
                    exchange(acc2, swap2, x2send, x2recv, k).start()
                for k in range(1, last):
                    exchange(acc2, swap2, x2send, x2recv, k).wait_recv()
                    acc2[k, mine] += swap2[k]
                    bring_home(acc2, ret2, r2send, r2recv, k).start()
                exchange(acc2, swap2, x2send, x2recv, 0).wait_recv()
                acc2[0, mine] = share[:, 0:1] * (acc2[0, mine] + swap2[0])

        for d in range(2, lines):
            pass_on(d, c)
            if d == 2:

                @pl.when(c < chunks - 1)
                def _():
                    send_own(c + 1)

                for k in range(2, chunks):

                    @pl.when(c == k - 2)
                    def _():
                        start_lend(k)

            add_both(d - 1, c)
        add_both(lines - 1, c)

        exchange(acc, swap, xsend, xrecv, c).start()
        exchange(acc, swap, xsend, xrecv, c).wait_recv()
        acc[c, mine] += swap[c]

        @pl.when(c > 0)
        def _():
            bring_home(acc, ret, rsend, rrecv, c).start()

        if assist:

            @pl.when(helper & (c == last))
            def _():
                for k in range(1, last):
                    bring_home(acc2, ret2, r2send, r2recv, k).wait_recv()
                    acc2[0, mine] += share[:, k : k + 1] * ret2[k]
                end_copy().start()

        return carry

    lax.fori_loop(0, chunks, chunk, 0)

    for j in range(lines):

        @pl.when(z != j)
        def _():
            remote(packed, states.at[j], ssend.at[j], srecv.at[j], (j, e)).wait_recv()

    gathered[...] = states[...]
    total = share[:, 0:1] * acc[0, mine]
    for c in range(1, chunks):
        bring_home(acc, ret, rsend, rrecv, c).wait_recv()
        total += share[:, c : c + 1] * ret[c]
    swap[0] = total
    if assist:

        @pl.when(edge)
        def _():
            end_copy().wait_recv()
            swap[0] += edge_in[...]

    out[...] = swap[0].astype(out.dtype)

    for j in range(lines):

        @pl.when(z != j)
        def _():
            state_copy(j).wait_send()

    if assist:

        @pl.when(edge)
        def _():
            for k in range(chunks):
                lend(k).wait_send()

        @pl.when(helper)
        def _():
            for k in range(last):
                exchange(acc2, swap2, x2send, x2recv, k).wait_send()
                if k > 0:
                    bring_home(acc2, ret2, r2send, r2recv, k).wait_send()
            end_copy().wait_send()

    for copy in copies:
        copy.wait_send()
    for c in range(chunks):
        for d in range(lines - 1):
            if assist and d == lines - 2 and c < last:
                continue

            @pl.when((z >= d) & (z < lines - 1))
            def _():
                to_right(d, c).wait_send()

            @pl.when((z + d < lines) & (z > 0))
            def _():
                to_left(d, c).wait_send()

        exchange(acc, swap, xsend, xrecv, c).wait_send()
        if c > 0:
            bring_home(acc, ret, rsend, rrecv, c).wait_send()


def expert_fused(packed, moe_tokens, expert_ids, route_weights, gate_proj, up_proj, down_proj):
    lines = lax.axis_size("ctx")
    chunks = GRID * GRID
    rows, width = moe_tokens.shape
    part = gate_proj.shape[2]
    columns = down_proj.shape[2]
    place = lax.axis_index("exp") // PAIR
    px, py = place % GRID, place // GRID
    order = jnp.stack(
        [((py + c // GRID) % GRID) * GRID + (px + c % GRID) % GRID for c in range(chunks)]
    )
    share = jnp.sum(
        jnp.where(expert_ids[:, :, None] == order[None, None, :], route_weights[:, :, None], 0.0),
        axis=1,
    )
    f32, bf16 = jnp.float32, jnp.bfloat16
    dma = pltpu.SemaphoreType.DMA
    vmem = pl.BlockSpec(memory_space=pltpu.VMEM)
    hbm = pl.BlockSpec(memory_space=pl.ANY)
    return pl.pallas_call(
        functools.partial(expert_kernel, lines),
        out_shape=(
            jax.ShapeDtypeStruct((rows, columns), bf16),
            jax.ShapeDtypeStruct((lines, *packed.shape), f32),
        ),
        in_specs=[vmem, vmem, vmem, hbm, hbm, hbm],
        out_specs=(vmem, vmem),
        scratch_shapes=[
            pltpu.VMEM((width, part), bf16),
            pltpu.VMEM((width, part), bf16),
            pltpu.VMEM((lines, part, columns), bf16),
            pltpu.VMEM((chunks, PAIR * rows, width), bf16),
            pltpu.VMEM((lines, chunks, PAIR * rows, part), bf16),
            pltpu.VMEM((chunks, PAIR * rows, columns), f32),
            pltpu.VMEM((chunks, rows, columns), f32),
            pltpu.VMEM((chunks, rows, columns), f32),
            pltpu.VMEM((part, columns), bf16),
            pltpu.VMEM((chunks - 1, PAIR * rows, columns), f32),
            pltpu.VMEM((chunks - 1, rows, columns), f32),
            pltpu.VMEM((chunks - 1, rows, columns), f32),
            pltpu.VMEM((rows, columns), f32),
            pltpu.VMEM((lines, *packed.shape), f32),
            dma((4,)),
            dma((8,)),
            dma((8,)),
            dma((lines, chunks)),
            dma((lines, chunks)),
            dma((lines, chunks)),
            dma((lines, chunks)),
            dma((chunks,)),
            dma((chunks,)),
            dma((chunks,)),
            dma((chunks,)),
            dma((lines,)),
            dma((lines,)),
            dma((chunks,)),
            dma((chunks,)),
            dma((chunks,)),
            dma((chunks,)),
            dma((chunks,)),
            dma((chunks,)),
            dma((1,)),
            dma((1,)),
        ],
        compiler_params=pltpu.CompilerParams(
            collective_id=0, has_side_effects=True, vmem_limit_bytes=VMEM_BYTES
        ),
    )(
        moe_tokens,
        share,
        packed,
        gate_proj[0],
        up_proj[0],
        down_proj[0].reshape(lines, part, columns),
    )


def expert_layer(packed, *arrays):
    moe_tokens, gate_proj, down_proj = arrays[0], arrays[3], arrays[5]
    if lax.axis_size("exp") == PAIR * GRID * GRID and gate_proj.shape[2] % 128 == 0:
        return expert_fused(packed, *arrays)
    return expert_block(*arrays), lax.all_gather(packed, "ctx")


def on_device(
    seq_inputs,
    step_size,
    write_map,
    read_map,
    decay_log,
    skip_gain,
    moe_tokens,
    expert_ids,
    route_weights,
    gate_proj,
    up_proj,
    down_proj,
):
    local_mix, cumulative, block_ends, entering, final = mixer_prepare(
        seq_inputs, step_size, write_map, read_map, decay_log
    )
    total_log = jnp.sum(block_ends, axis=1)
    head_count, state_count, head_width = final.shape
    logs = jnp.broadcast_to(total_log[:, None, None], (head_count, 8, head_width))
    packed = jnp.concatenate([final, logs], axis=1)
    expert_output, gathered = expert_layer(
        packed, moe_tokens, expert_ids, route_weights, gate_proj, up_proj, down_proj
    )
    place = lax.axis_index("ctx")
    state_before = jnp.zeros_like(final)
    for lap in range(lax.axis_size("ctx")):
        latter = gathered[lap]
        decay = jnp.exp(latter[:, state_count, 0])
        added = decay[:, None, None] * state_before + latter[:, :state_count]
        state_before = jnp.where(lap < place, added, state_before)
    mixer_output = mixer_finish(
        local_mix, cumulative, block_ends, entering, state_before, read_map, seq_inputs, skip_gain
    )
    return (mixer_output, expert_output)


def solution(mesh):
    return jax.shard_map(
        on_device,
        mesh=mesh,
        in_specs=(
            P("ctx", "exp"),
            P("exp", "ctx"),
            P(None, "ctx"),
            P(None, "ctx"),
            P("exp"),
            P("exp"),
            P("exp", None),
            P("exp", None),
            P("exp", None),
            P("exp", None, "ctx"),
            P("exp", None, "ctx"),
            P("exp", None, "ctx"),
        ),
        out_specs=(P("ctx", "exp"), P("exp", "ctx")),
        check_vma=False,
    )
```

```python
import functools

import jax
import jax.numpy as jnp
from jax import lax
from jax.experimental import pallas as pl
from jax.experimental.pallas import tpu as pltpu
from jax.sharding import PartitionSpec as P

BLOCK = 256


HIGHEST = lax.Precision.HIGHEST


def block_chain(running, pieces):
    decay, increment = pieces
    return (decay[:, None, None] * running + increment, running)


def mixer_prepare(seq_inputs, step_size, write_map, read_map, decay_log):
    length = seq_inputs.shape[0]
    head_count = step_size.shape[0]
    state_count = write_map.shape[0]
    head_width = seq_inputs.shape[1] // head_count
    block_count = length // BLOCK
    decay_rate = -jnp.exp(decay_log)
    log_decay = (step_size * decay_rate[:, None]).reshape(head_count, block_count, BLOCK)
    order = lax.broadcasted_iota(jnp.int32, (BLOCK, BLOCK), 0)
    until = (order <= lax.broadcasted_iota(jnp.int32, (BLOCK, BLOCK), 1)).astype(jnp.float32)
    cumulative = jnp.einsum("hks,st->hkt", log_decay, until, precision=HIGHEST)
    block_ends = cumulative[:, :, BLOCK - 1]
    step_blocks = step_size.reshape(head_count, block_count, BLOCK)
    write_blocks = write_map.reshape(state_count, block_count, BLOCK)
    read_blocks = read_map.reshape(state_count, block_count, BLOCK)
    value_blocks = seq_inputs.reshape(block_count, BLOCK, head_count, head_width)
    scores = jnp.einsum(
        "nkt,nks->kts", read_blocks, write_blocks, preferred_element_type=jnp.float32
    )
    row_index = lax.broadcasted_iota(jnp.int32, (BLOCK, BLOCK), 0)
    column_index = lax.broadcasted_iota(jnp.int32, (BLOCK, BLOCK), 1)
    lower = column_index <= row_index
    difference = cumulative[:, :, :, None] - cumulative[:, :, None, :]
    decay = jnp.where(lower[None, None], jnp.exp(jnp.minimum(difference, 0.0)), 0.0)
    mixing = (scores[None] * decay * step_blocks[:, :, None, :]).astype(jnp.bfloat16)
    local_mix = jnp.einsum(
        "hkts,kshp->kthp", mixing, value_blocks, preferred_element_type=jnp.float32
    )
    weights = jnp.exp(block_ends[:, :, None] - cumulative) * step_blocks
    key_decayed = (write_blocks[None] * weights[:, None]).astype(jnp.bfloat16)
    increments = jnp.einsum(
        "hnks,kshp->khnp", key_decayed, value_blocks, preferred_element_type=jnp.float32
    )
    zero_state = jnp.zeros((head_count, state_count, head_width), jnp.float32)
    final, entering = lax.scan(block_chain, zero_state, (jnp.exp(block_ends).T, increments))
    return (local_mix, cumulative, block_ends, entering, final)


def mixer_finish(
    local_mix, cumulative, block_ends, entering, state_before, read_map, seq_inputs, skip_gain
):
    head_count = block_ends.shape[0]
    block_count = block_ends.shape[1]
    state_count = read_map.shape[0]
    head_width = entering.shape[3]
    before = jnp.cumsum(block_ends, axis=1) - block_ends
    states = jnp.exp(before).T[:, :, None, None] * state_before[None] + entering
    read_blocks = read_map.reshape(state_count, block_count, BLOCK).astype(jnp.float32)
    carried = jnp.einsum("nkt,khnp->kthp", read_blocks, states, precision=HIGHEST)
    carried = carried * jnp.exp(cumulative).transpose(1, 2, 0)[:, :, :, None]
    value_blocks = seq_inputs.reshape(block_count, BLOCK, head_count, head_width).astype(
        jnp.float32
    )
    output = local_mix + carried + skip_gain[None, None, :, None] * value_blocks
    return output.reshape(seq_inputs.shape).astype(jnp.bfloat16)


def expert_block(moe_tokens, expert_ids, route_weights, gate_proj, up_proj, down_proj):
    group_size = moe_tokens.shape[0]
    model_width = moe_tokens.shape[1]
    expert_count = lax.axis_size("exp") // 2
    capacity = min(group_size, 4 * group_size // expert_count)
    slot_count = expert_count * capacity
    assigned = expert_ids.reshape(group_size * 2)
    onehot = (
        assigned[:, None] == lax.broadcasted_iota(jnp.int32, (group_size * 2, expert_count), 1)
    ).astype(jnp.int32)
    earlier_count = jnp.cumsum(onehot, axis=0) - onehot
    position = jnp.sum((earlier_count + assigned[:, None] * capacity) * onehot, axis=1)
    matches = (
        position[:, None] == lax.broadcasted_iota(jnp.int32, (group_size * 2, slot_count), 1)
    ).astype(jnp.float32)
    dispatch = jnp.sum(matches.reshape(group_size, 2, slot_count), axis=1).astype(jnp.bfloat16)
    combine = jnp.sum(
        (matches * route_weights.reshape(group_size * 2)[:, None]).reshape(
            group_size, 2, slot_count
        ),
        axis=1,
    )
    gate_weight = gate_proj[0]
    up_weight = up_proj[0]
    down_weight = down_proj[0]
    packed = jnp.einsum(
        "is,id->sd", dispatch, moe_tokens, preferred_element_type=jnp.float32
    ).astype(jnp.bfloat16)
    doubled = jnp.broadcast_to(
        packed.reshape(expert_count, 1, capacity, model_width),
        (expert_count, 2, capacity, model_width),
    )
    arrived = lax.all_to_all(
        doubled.reshape(2 * slot_count, model_width), "exp", split_axis=0, concat_axis=0, tiled=True
    )
    gate_sums = jnp.dot(arrived, gate_weight, preferred_element_type=jnp.float32)
    up_sums = jnp.dot(arrived, up_weight, preferred_element_type=jnp.float32)
    hidden = (jax.nn.silu(gate_sums) * up_sums).astype(jnp.bfloat16)
    partial_out = jnp.dot(
        lax.all_gather(hidden, "ctx", axis=1, tiled=True),
        down_weight,
        preferred_element_type=jnp.float32,
    )
    returned = lax.all_to_all(partial_out, "exp", split_axis=0, concat_axis=0, tiled=True)
    summed = jnp.sum(returned.reshape(expert_count, 2, capacity, -1), axis=1).reshape(
        slot_count, -1
    )
    result = jnp.dot(combine, summed, precision=HIGHEST, preferred_element_type=jnp.float32)
    return result.astype(jnp.bfloat16)


MESH = pl.DeviceIdType.MESH
VMEM_BYTES = 60 * 2**20
GRID = 2
PAIR = 2


def expert_kernel(
    lines,
    tok_in,
    share,
    packed,
    gate_hbm,
    up_hbm,
    down_hbm,
    out,
    gathered,
    gate_w,
    up_w,
    down_w,
    tok,
    hid,
    acc,
    swap,
    ret,
    far_w,
    acc2,
    swap2,
    ret2,
    edge_in,
    states,
    load_sem,
    tsend,
    trecv,
    hsend_r,
    hsend_l,
    hrecv_l,
    hrecv_r,
    xsend,
    xrecv,
    rsend,
    rrecv,
    ssend,
    srecv,
    wsend,
    wrecv,
    x2send,
    x2recv,
    r2send,
    r2recv,
    esend,
    erecv,
):
    chunks = GRID * GRID
    z = lax.axis_index("ctx")
    e = lax.axis_index("exp")
    half = lax.rem(e, PAIR)
    other = 1 - half
    px = lax.rem(e // PAIR, GRID)
    py = e // (PAIR * GRID)
    rows = tok_in.shape[0]
    sub = rows // 2

    def peer(c, core):
        qx = lax.rem(px + lax.rem(c, GRID), GRID)
        qy = lax.rem(py + c // GRID, GRID)
        return (z, (qy * GRID + qx) * PAIR + core)

    mine = pl.ds(pl.multiple_of(half * rows, rows), rows)
    theirs = pl.ds(pl.multiple_of(other * rows, rows), rows)
    partner = (z, (py * GRID + px) * PAIR + other)

    loads = [
        pltpu.make_async_copy(gate_hbm, gate_w, load_sem.at[0]),
        pltpu.make_async_copy(up_hbm, up_w, load_sem.at[1]),
        pltpu.make_async_copy(tok_in, tok.at[0, mine], load_sem.at[3]),
        pltpu.make_async_copy(down_hbm, down_w, load_sem.at[2]),
    ]
    for load in loads[:3]:
        load.start()

    barrier = pltpu.get_barrier_semaphore()
    for device in (partner, peer(1, half), peer(2, half), peer(3, half)):
        pl.semaphore_signal(barrier, inc=1, device_id=device, device_id_type=MESH)

    for j in range(lines):

        @pl.when(z != j)
        def _():
            pl.semaphore_signal(barrier, inc=1, device_id=(j, e), device_id_type=MESH)

    pl.semaphore_wait(barrier, 4 + lines - 1)

    def remote(src, dst, ssem, rsem, device):
        return pltpu.make_async_remote_copy(
            src_ref=src,
            dst_ref=dst,
            send_sem=ssem,
            recv_sem=rsem,
            device_id=device,
            device_id_type=MESH,
        )

    upper = pl.ds(pl.multiple_of(half * rows, rows), sub)
    lower = pl.ds(pl.multiple_of(half * rows + sub, sub), sub)
    copies = [
        remote(tok_in, tok.at[0, mine], tsend.at[0], trecv.at[0], partner),
        remote(tok_in, tok.at[1, mine], tsend.at[1], trecv.at[1], peer(1, half)),
        remote(tok_in, tok.at[2, mine], tsend.at[2], trecv.at[2], peer(2, half)),
        remote(
            tok.at[1, upper], tok.at[3, upper], tsend.at[3], trecv.at[3], peer(2, half)
        ),
        remote(
            tok.at[2, lower], tok.at[3, lower], tsend.at[4], trecv.at[4], peer(1, half)
        ),
        remote(tok.at[1, mine], tok.at[1, mine], tsend.at[5], trecv.at[5], partner),
        remote(tok.at[2, mine], tok.at[2, mine], tsend.at[6], trecv.at[6], partner),
        remote(tok.at[3, mine], tok.at[3, mine], tsend.at[7], trecv.at[7], partner),
    ]
    for copy in copies[:3]:
        copy.start()

    last = chunks - 1
    assist = lines > 3
    edge = (z == 0) | (z == lines - 1)
    helper = (z == 1) | (z == lines - 2)
    far = jnp.where(z < 2, lines - 1, 0)
    piece = far_w.shape[0] // chunks

    def lend(k):
        span = pl.ds(k * piece, piece)
        target = jnp.where(z == 0, 1, lines - 2)
        return remote(
            down_hbm.at[far, span], far_w.at[span], wsend.at[k], wrecv.at[k], (target, e)
        )

    def start_lend(k):
        if assist:

            @pl.when(edge)
            def _():
                lend(k).start()

    def state_copy(j):
        return remote(packed, states.at[z], ssend.at[j], srecv.at[z], (j, e))

    start_lend(0)
    for j in range(lines):

        @pl.when(z != j)
        def _():
            state_copy(j).start()

    states[z] = packed[...]

    def make_hidden(c):
        width = gate_w.shape[1]
        x = tok[c]
        g = jnp.dot(x, gate_w[...], preferred_element_type=jnp.float32)
        u = jnp.dot(x, up_w[...], preferred_element_type=jnp.float32)
        hid[z, c] = (jax.nn.silu(g) * u).astype(jnp.bfloat16)

    def to_right(d, c):
        j = z - d
        return remote(hid.at[j, c], hid.at[j, c], hsend_r.at[d, c], hrecv_l.at[d, c], (z + 1, e))

    def to_left(d, c):
        j = z + d
        return remote(hid.at[j, c], hid.at[j, c], hsend_l.at[d, c], hrecv_r.at[d, c], (z - 1, e))

    def from_left(d, c):
        return remote(
            hid.at[z - d, c], hid.at[z - d, c], hsend_r.at[d, c], hrecv_l.at[d - 1, c], (z - 1, e)
        )

    def from_right(d, c):
        return remote(
            hid.at[z + d, c], hid.at[z + d, c], hsend_l.at[d, c], hrecv_r.at[d - 1, c], (z + 1, e)
        )

    def send_own(c):
        @pl.when(z < lines - 1)
        def _():
            to_right(0, c).start()

        @pl.when(z > 0)
        def _():
            to_left(0, c).start()

    def needed(d, c):
        return (c == last) if assist and d == lines - 1 else True

    def pass_rightward(d, c, turn):
        @pl.when((z >= d) & needed(d, c) & turn)
        def _():
            from_left(d, c).wait_recv()

            @pl.when((z < lines - 1) & needed(d + 1, c))
            def _():
                to_right(d, c).start()

    def pass_leftward(d, c, turn):
        @pl.when((z + d < lines) & needed(d, c) & turn)
        def _():
            from_right(d, c).wait_recv()

            @pl.when((z > 0) & needed(d + 1, c))
            def _():
                to_left(d, c).start()

    low = z < lines // 2

    def pass_first(d, c):
        pass_leftward(d, c, low)
        pass_rightward(d, c, jnp.logical_not(low))

    def pass_second(d, c):
        pass_rightward(d, c, low)
        pass_leftward(d, c, jnp.logical_not(low))

    def add_down(j, c):
        acc[c] += jnp.dot(hid[j, c], down_w[j], preferred_element_type=jnp.float32)

    def add_both(d, c):
        @pl.when((z >= d) & needed(d, c))
        def _():
            add_down(z - d, c)

        @pl.when((z + d < lines) & needed(d, c))
        def _():
            add_down(z + d, c)

    def exchange(total, landing, ssem, rsem, c):
        return remote(total.at[c, theirs], landing.at[c], ssem.at[c], rsem.at[c], partner)

    def bring_home(total, landing, ssem, rsem, c):
        return remote(total.at[c, mine], landing.at[c], ssem.at[c], rsem.at[c], peer(c, half))

    def end_copy():
        target = jnp.where(z == 1, 0, lines - 1)
        return remote(acc2.at[0, mine], edge_in, esend.at[0], erecv.at[0], (target, e))

    loads[2].wait()
    loads[0].wait()
    loads[1].wait()
    loads[3].start()
    copies[0].wait_recv()
    make_hidden(0)
    send_own(0)
    start_lend(1)
    loads[3].wait()

    def chunk(c, carry):
        acc[c] = jnp.dot(hid[z, c], down_w[z], preferred_element_type=jnp.float32)
        pass_first(1, c)

        @pl.when(c == 0)
        def _():
            copies[1].wait_recv()
            copies[5].start()
            copies[3].start()
            copies[2].wait_recv()
            copies[6].start()
            copies[4].start()
            copies[5].wait_recv()

        @pl.when(c == 1)
        def _():
            copies[3].wait_recv()
            copies[4].wait_recv()
            copies[7].start()
            copies[6].wait_recv()

        @pl.when(c == 2)
        def _():
            copies[7].wait_recv()

        @pl.when(c < chunks - 1)
        def _():
            make_hidden(c + 1)
            send_own(c + 1)

        for k in range(2, chunks):

            @pl.when(c == k - 2)
            def _():
                start_lend(k)

        pass_second(1, c)

        if assist:

            @pl.when(helper & (c == last))
            def _():
                for k in range(chunks):
                    lend(k).wait_recv()
                for k in range(last):
                    acc2[k] = jnp.dot(
                        hid[far, k], far_w[...], preferred_element_type=jnp.float32
                    )
                    exchange(acc2, swap2, x2send, x2recv, k).start()
                for k in range(1, last):
                    exchange(acc2, swap2, x2send, x2recv, k).wait_recv()
                    acc2[k, mine] += swap2[k]
                    bring_home(acc2, ret2, r2send, r2recv, k).start()
                exchange(acc2, swap2, x2send, x2recv, 0).wait_recv()
                acc2[0, mine] = share[:, 0:1] * (acc2[0, mine] + swap2[0])

        for d in range(2, lines):
            pass_first(d, c)
            pass_second(d, c)
            add_both(d - 1, c)
        add_both(lines - 1, c)

        exchange(acc, swap, xsend, xrecv, c).start()
        exchange(acc, swap, xsend, xrecv, c).wait_recv()
        acc[c, mine] += swap[c]

        @pl.when(c > 0)
        def _():
            bring_home(acc, ret, rsend, rrecv, c).start()

        if assist:

            @pl.when(helper & (c == last))
            def _():
                for k in range(1, last):
                    bring_home(acc2, ret2, r2send, r2recv, k).wait_recv()
                    acc2[0, mine] += share[:, k : k + 1] * ret2[k]
                end_copy().start()

        return carry

    lax.fori_loop(0, chunks, chunk, 0)

    for j in range(lines):

        @pl.when(z != j)
        def _():
            remote(packed, states.at[j], ssend.at[j], srecv.at[j], (j, e)).wait_recv()

    gathered[...] = states[...]
    total = share[:, 0:1] * acc[0, mine]
    for c in range(1, chunks):
        bring_home(acc, ret, rsend, rrecv, c).wait_recv()
        total += share[:, c : c + 1] * ret[c]
    swap[0] = total
    if assist:

        @pl.when(edge)
        def _():
            end_copy().wait_recv()
            swap[0] += edge_in[...]

    out[...] = swap[0].astype(out.dtype)

    for j in range(lines):

        @pl.when(z != j)
        def _():
            state_copy(j).wait_send()

    if assist:

        @pl.when(edge)
        def _():
            for k in range(chunks):
                lend(k).wait_send()

        @pl.when(helper)
        def _():
            for k in range(last):
                exchange(acc2, swap2, x2send, x2recv, k).wait_send()
                if k > 0:
                    bring_home(acc2, ret2, r2send, r2recv, k).wait_send()
            end_copy().wait_send()

    for copy in copies:
        copy.wait_send()
    for c in range(chunks):
        for d in range(lines - 1):
            if assist and d == lines - 2 and c < last:
                continue

            @pl.when((z >= d) & (z < lines - 1))
            def _():
                to_right(d, c).wait_send()

            @pl.when((z + d < lines) & (z > 0))
            def _():
                to_left(d, c).wait_send()

        exchange(acc, swap, xsend, xrecv, c).wait_send()
        if c > 0:
            bring_home(acc, ret, rsend, rrecv, c).wait_send()


def expert_fused(packed, moe_tokens, expert_ids, route_weights, gate_proj, up_proj, down_proj):
    lines = lax.axis_size("ctx")
    chunks = GRID * GRID
    rows, width = moe_tokens.shape
    part = gate_proj.shape[2]
    columns = down_proj.shape[2]
    place = lax.axis_index("exp") // PAIR
    px, py = place % GRID, place // GRID
    order = jnp.stack(
        [((py + c // GRID) % GRID) * GRID + (px + c % GRID) % GRID for c in range(chunks)]
    )
    share = jnp.sum(
        jnp.where(expert_ids[:, :, None] == order[None, None, :], route_weights[:, :, None], 0.0),
        axis=1,
    )
    f32, bf16 = jnp.float32, jnp.bfloat16
    dma = pltpu.SemaphoreType.DMA
    vmem = pl.BlockSpec(memory_space=pltpu.VMEM)
    hbm = pl.BlockSpec(memory_space=pl.ANY)
    return pl.pallas_call(
        functools.partial(expert_kernel, lines),
        out_shape=(
            jax.ShapeDtypeStruct((rows, columns), bf16),
            jax.ShapeDtypeStruct((lines, *packed.shape), f32),
        ),
        in_specs=[vmem, vmem, vmem, hbm, hbm, hbm],
        out_specs=(vmem, vmem),
        scratch_shapes=[
            pltpu.VMEM((width, part), bf16),
            pltpu.VMEM((width, part), bf16),
            pltpu.VMEM((lines, part, columns), bf16),
            pltpu.VMEM((chunks, PAIR * rows, width), bf16),
            pltpu.VMEM((lines, chunks, PAIR * rows, part), bf16),
            pltpu.VMEM((chunks, PAIR * rows, columns), f32),
            pltpu.VMEM((chunks, rows, columns), f32),
            pltpu.VMEM((chunks, rows, columns), f32),
            pltpu.VMEM((part, columns), bf16),
            pltpu.VMEM((chunks - 1, PAIR * rows, columns), f32),
            pltpu.VMEM((chunks - 1, rows, columns), f32),
            pltpu.VMEM((chunks - 1, rows, columns), f32),
            pltpu.VMEM((rows, columns), f32),
            pltpu.VMEM((lines, *packed.shape), f32),
            dma((4,)),
            dma((8,)),
            dma((8,)),
            dma((lines, chunks)),
            dma((lines, chunks)),
            dma((lines, chunks)),
            dma((lines, chunks)),
            dma((chunks,)),
            dma((chunks,)),
            dma((chunks,)),
            dma((chunks,)),
            dma((lines,)),
            dma((lines,)),
            dma((chunks,)),
            dma((chunks,)),
            dma((chunks,)),
            dma((chunks,)),
            dma((chunks,)),
            dma((chunks,)),
            dma((1,)),
            dma((1,)),
        ],
        compiler_params=pltpu.CompilerParams(
            collective_id=0, has_side_effects=True, vmem_limit_bytes=VMEM_BYTES
        ),
    )(
        moe_tokens,
        share,
        packed,
        gate_proj[0],
        up_proj[0],
        down_proj[0].reshape(lines, part, columns),
    )


def expert_layer(packed, *arrays):
    moe_tokens, gate_proj, down_proj = arrays[0], arrays[3], arrays[5]
    if lax.axis_size("exp") == PAIR * GRID * GRID and gate_proj.shape[2] % 128 == 0:
        return expert_fused(packed, *arrays)
    return expert_block(*arrays), lax.all_gather(packed, "ctx")


def on_device(
    seq_inputs,
    step_size,
    write_map,
    read_map,
    decay_log,
    skip_gain,
    moe_tokens,
    expert_ids,
    route_weights,
    gate_proj,
    up_proj,
    down_proj,
):
    local_mix, cumulative, block_ends, entering, final = mixer_prepare(
        seq_inputs, step_size, write_map, read_map, decay_log
    )
    total_log = jnp.sum(block_ends, axis=1)
    head_count, state_count, head_width = final.shape
    logs = jnp.broadcast_to(total_log[:, None, None], (head_count, 8, head_width))
    packed = jnp.concatenate([final, logs], axis=1)
    expert_output, gathered = expert_layer(
        packed, moe_tokens, expert_ids, route_weights, gate_proj, up_proj, down_proj
    )
    place = lax.axis_index("ctx")
    state_before = jnp.zeros_like(final)
    for lap in range(lax.axis_size("ctx")):
        latter = gathered[lap]
        decay = jnp.exp(latter[:, state_count, 0])
        added = decay[:, None, None] * state_before + latter[:, :state_count]
        state_before = jnp.where(lap < place, added, state_before)
    mixer_output = mixer_finish(
        local_mix, cumulative, block_ends, entering, state_before, read_map, seq_inputs, skip_gain
    )
    return (mixer_output, expert_output)


def solution(mesh):
    return jax.shard_map(
        on_device,
        mesh=mesh,
        in_specs=(
            P("ctx", "exp"),
            P("exp", "ctx"),
            P(None, "ctx"),
            P(None, "ctx"),
            P("exp"),
            P("exp"),
            P("exp", None),
            P("exp", None),
            P("exp", None),
            P("exp", None, "ctx"),
            P("exp", None, "ctx"),
            P("exp", None, "ctx"),
        ),
        out_specs=(P("ctx", "exp"), P("exp", "ctx")),
        check_vma=False,
    )
```

```python
import functools

import jax
import jax.numpy as jnp
from jax import lax
from jax.experimental import pallas as pl
from jax.experimental.pallas import tpu as pltpu
from jax.sharding import PartitionSpec as P

BLOCK = 256


HIGHEST = lax.Precision.HIGHEST


def block_chain(running, pieces):
    decay, increment = pieces
    return (decay[:, None, None] * running + increment, running)


def mixer_prepare(seq_inputs, step_size, write_map, read_map, decay_log):
    length = seq_inputs.shape[0]
    head_count = step_size.shape[0]
    state_count = write_map.shape[0]
    head_width = seq_inputs.shape[1] // head_count
    block_count = length // BLOCK
    decay_rate = -jnp.exp(decay_log)
    log_decay = (step_size * decay_rate[:, None]).reshape(head_count, block_count, BLOCK)
    order = lax.broadcasted_iota(jnp.int32, (BLOCK, BLOCK), 0)
    until = (order <= lax.broadcasted_iota(jnp.int32, (BLOCK, BLOCK), 1)).astype(jnp.float32)
    cumulative = jnp.einsum("hks,st->hkt", log_decay, until, precision=HIGHEST)
    block_ends = cumulative[:, :, BLOCK - 1]
    step_blocks = step_size.reshape(head_count, block_count, BLOCK)
    write_blocks = write_map.reshape(state_count, block_count, BLOCK)
    read_blocks = read_map.reshape(state_count, block_count, BLOCK)
    value_blocks = seq_inputs.reshape(block_count, BLOCK, head_count, head_width)
    scores = jnp.einsum(
        "nkt,nks->kts", read_blocks, write_blocks, preferred_element_type=jnp.float32
    )
    row_index = lax.broadcasted_iota(jnp.int32, (BLOCK, BLOCK), 0)
    column_index = lax.broadcasted_iota(jnp.int32, (BLOCK, BLOCK), 1)
    lower = column_index <= row_index
    difference = cumulative[:, :, :, None] - cumulative[:, :, None, :]
    decay = jnp.where(lower[None, None], jnp.exp(jnp.minimum(difference, 0.0)), 0.0)
    mixing = (scores[None] * decay * step_blocks[:, :, None, :]).astype(jnp.bfloat16)
    local_mix = jnp.einsum(
        "hkts,kshp->kthp", mixing, value_blocks, preferred_element_type=jnp.float32
    )
    weights = jnp.exp(block_ends[:, :, None] - cumulative) * step_blocks
    key_decayed = (write_blocks[None] * weights[:, None]).astype(jnp.bfloat16)
    increments = jnp.einsum(
        "hnks,kshp->khnp", key_decayed, value_blocks, preferred_element_type=jnp.float32
    )
    zero_state = jnp.zeros((head_count, state_count, head_width), jnp.float32)
    final, entering = lax.scan(block_chain, zero_state, (jnp.exp(block_ends).T, increments))
    return (local_mix, cumulative, block_ends, entering, final)


def mixer_finish(
    local_mix, cumulative, block_ends, entering, state_before, read_map, seq_inputs, skip_gain
):
    head_count = block_ends.shape[0]
    block_count = block_ends.shape[1]
    state_count = read_map.shape[0]
    head_width = entering.shape[3]
    before = jnp.cumsum(block_ends, axis=1) - block_ends
    states = jnp.exp(before).T[:, :, None, None] * state_before[None] + entering
    read_blocks = read_map.reshape(state_count, block_count, BLOCK).astype(jnp.float32)
    carried = jnp.einsum("nkt,khnp->kthp", read_blocks, states, precision=HIGHEST)
    carried = carried * jnp.exp(cumulative).transpose(1, 2, 0)[:, :, :, None]
    value_blocks = seq_inputs.reshape(block_count, BLOCK, head_count, head_width).astype(
        jnp.float32
    )
    output = local_mix + carried + skip_gain[None, None, :, None] * value_blocks
    return output.reshape(seq_inputs.shape).astype(jnp.bfloat16)


def expert_block(moe_tokens, expert_ids, route_weights, gate_proj, up_proj, down_proj):
    group_size = moe_tokens.shape[0]
    model_width = moe_tokens.shape[1]
    expert_count = lax.axis_size("exp") // 2
    capacity = min(group_size, 4 * group_size // expert_count)
    slot_count = expert_count * capacity
    assigned = expert_ids.reshape(group_size * 2)
    onehot = (
        assigned[:, None] == lax.broadcasted_iota(jnp.int32, (group_size * 2, expert_count), 1)
    ).astype(jnp.int32)
    earlier_count = jnp.cumsum(onehot, axis=0) - onehot
    position = jnp.sum((earlier_count + assigned[:, None] * capacity) * onehot, axis=1)
    matches = (
        position[:, None] == lax.broadcasted_iota(jnp.int32, (group_size * 2, slot_count), 1)
    ).astype(jnp.float32)
    dispatch = jnp.sum(matches.reshape(group_size, 2, slot_count), axis=1).astype(jnp.bfloat16)
    combine = jnp.sum(
        (matches * route_weights.reshape(group_size * 2)[:, None]).reshape(
            group_size, 2, slot_count
        ),
        axis=1,
    )
    gate_weight = gate_proj[0]
    up_weight = up_proj[0]
    down_weight = down_proj[0]
    packed = jnp.einsum(
        "is,id->sd", dispatch, moe_tokens, preferred_element_type=jnp.float32
    ).astype(jnp.bfloat16)
    doubled = jnp.broadcast_to(
        packed.reshape(expert_count, 1, capacity, model_width),
        (expert_count, 2, capacity, model_width),
    )
    arrived = lax.all_to_all(
        doubled.reshape(2 * slot_count, model_width), "exp", split_axis=0, concat_axis=0, tiled=True
    )
    gate_sums = jnp.dot(arrived, gate_weight, preferred_element_type=jnp.float32)
    up_sums = jnp.dot(arrived, up_weight, preferred_element_type=jnp.float32)
    hidden = (jax.nn.silu(gate_sums) * up_sums).astype(jnp.bfloat16)
    partial_out = jnp.dot(
        lax.all_gather(hidden, "ctx", axis=1, tiled=True),
        down_weight,
        preferred_element_type=jnp.float32,
    )
    returned = lax.all_to_all(partial_out, "exp", split_axis=0, concat_axis=0, tiled=True)
    summed = jnp.sum(returned.reshape(expert_count, 2, capacity, -1), axis=1).reshape(
        slot_count, -1
    )
    result = jnp.dot(combine, summed, precision=HIGHEST, preferred_element_type=jnp.float32)
    return result.astype(jnp.bfloat16)


MESH = pl.DeviceIdType.MESH
VMEM_BYTES = 60 * 2**20
GRID = 2
PAIR = 2


def expert_kernel(
    lines,
    tok_in,
    share,
    packed,
    gate_hbm,
    up_hbm,
    down_hbm,
    out,
    gathered,
    gate_w,
    up_w,
    down_w,
    tok,
    hid,
    acc,
    swap,
    ret,
    far_w,
    acc2,
    swap2,
    ret2,
    edge_in,
    states,
    load_sem,
    tsend,
    trecv,
    hsend_r,
    hsend_l,
    hrecv_l,
    hrecv_r,
    xsend,
    xrecv,
    rsend,
    rrecv,
    ssend,
    srecv,
    wsend,
    wrecv,
    x2send,
    x2recv,
    r2send,
    r2recv,
    esend,
    erecv,
):
    chunks = GRID * GRID
    z = lax.axis_index("ctx")
    e = lax.axis_index("exp")
    half = lax.rem(e, PAIR)
    other = 1 - half
    px = lax.rem(e // PAIR, GRID)
    py = e // (PAIR * GRID)
    rows = tok_in.shape[0]
    sub = rows // 2

    def peer(c, core):
        qx = lax.rem(px + lax.rem(c, GRID), GRID)
        qy = lax.rem(py + c // GRID, GRID)
        return (z, (qy * GRID + qx) * PAIR + core)

    mine = pl.ds(pl.multiple_of(half * rows, rows), rows)
    theirs = pl.ds(pl.multiple_of(other * rows, rows), rows)
    partner = (z, (py * GRID + px) * PAIR + other)

    loads = [
        pltpu.make_async_copy(gate_hbm, gate_w, load_sem.at[0]),
        pltpu.make_async_copy(up_hbm, up_w, load_sem.at[1]),
        pltpu.make_async_copy(tok_in, tok.at[0, mine], load_sem.at[3]),
        pltpu.make_async_copy(down_hbm, down_w, load_sem.at[2]),
    ]
    for load in loads[:3]:
        load.start()

    barrier = pltpu.get_barrier_semaphore()
    for device in (partner, peer(1, half), peer(2, half), peer(3, half)):
        pl.semaphore_signal(barrier, inc=1, device_id=device, device_id_type=MESH)

    for j in range(lines):

        @pl.when(z != j)
        def _():
            pl.semaphore_signal(barrier, inc=1, device_id=(j, e), device_id_type=MESH)

    pl.semaphore_wait(barrier, 4 + lines - 1)

    def remote(src, dst, ssem, rsem, device):
        return pltpu.make_async_remote_copy(
            src_ref=src,
            dst_ref=dst,
            send_sem=ssem,
            recv_sem=rsem,
            device_id=device,
            device_id_type=MESH,
        )

    upper = pl.ds(pl.multiple_of(half * rows, rows), sub)
    lower = pl.ds(pl.multiple_of(half * rows + sub, sub), sub)
    copies = [
        remote(tok_in, tok.at[0, mine], tsend.at[0], trecv.at[0], partner),
        remote(tok_in, tok.at[1, mine], tsend.at[1], trecv.at[1], peer(1, half)),
        remote(tok_in, tok.at[2, mine], tsend.at[2], trecv.at[2], peer(2, half)),
        remote(
            tok.at[1, upper], tok.at[3, upper], tsend.at[3], trecv.at[3], peer(2, half)
        ),
        remote(
            tok.at[2, lower], tok.at[3, lower], tsend.at[4], trecv.at[4], peer(1, half)
        ),
        remote(tok.at[1, mine], tok.at[1, mine], tsend.at[5], trecv.at[5], partner),
        remote(tok.at[2, mine], tok.at[2, mine], tsend.at[6], trecv.at[6], partner),
        remote(tok.at[3, mine], tok.at[3, mine], tsend.at[7], trecv.at[7], partner),
    ]
    for copy in copies[:3]:
        copy.start()

    last = chunks - 1
    assist = lines > 3
    edge = (z == 0) | (z == lines - 1)
    helper = (z == 1) | (z == lines - 2)
    far = jnp.where(z < 2, lines - 1, 0)
    piece = far_w.shape[0] // chunks

    def lend(k):
        span = pl.ds(k * piece, piece)
        target = jnp.where(z == 0, 1, lines - 2)
        return remote(
            down_hbm.at[far, span], far_w.at[span], wsend.at[k], wrecv.at[k], (target, e)
        )

    def start_lend(k):
        if assist:

            @pl.when(edge)
            def _():
                lend(k).start()

    def state_copy(j):
        return remote(packed, states.at[z], ssend.at[j], srecv.at[z], (j, e))

    start_lend(0)
    for j in range(lines):

        @pl.when(z != j)
        def _():
            state_copy(j).start()

    states[z] = packed[...]

    def make_hidden(c):
        width = gate_w.shape[1]
        x = tok[c]
        g = jnp.dot(x, gate_w[...], preferred_element_type=jnp.float32)
        u = jnp.dot(x, up_w[...], preferred_element_type=jnp.float32)
        hid[z, c] = (jax.nn.silu(g) * u).astype(jnp.bfloat16)

    def to_right(d, c):
        j = z - d
        return remote(hid.at[j, c], hid.at[j, c], hsend_r.at[d, c], hrecv_l.at[d, c], (z + 1, e))

    def to_left(d, c):
        j = z + d
        return remote(hid.at[j, c], hid.at[j, c], hsend_l.at[d, c], hrecv_r.at[d, c], (z - 1, e))

    def from_left(d, c):
        return remote(
            hid.at[z - d, c], hid.at[z - d, c], hsend_r.at[d, c], hrecv_l.at[d - 1, c], (z - 1, e)
        )

    def from_right(d, c):
        return remote(
            hid.at[z + d, c], hid.at[z + d, c], hsend_l.at[d, c], hrecv_r.at[d - 1, c], (z + 1, e)
        )

    def send_own(c):
        @pl.when(z < lines - 1)
        def _():
            to_right(0, c).start()

        @pl.when(z > 0)
        def _():
            to_left(0, c).start()

    def needed(d, c):
        return (c == last) if assist and d == lines - 1 else True

    def pass_on(d, c):
        @pl.when((z >= d) & needed(d, c))
        def _():
            from_left(d, c).wait_recv()

            @pl.when((z < lines - 1) & needed(d + 1, c))
            def _():
                to_right(d, c).start()

        @pl.when((z + d < lines) & needed(d, c))
        def _():
            from_right(d, c).wait_recv()

            @pl.when((z > 0) & needed(d + 1, c))
            def _():
                to_left(d, c).start()

    def add_down(j, c):
        acc[c] += jnp.dot(hid[j, c], down_w[j], preferred_element_type=jnp.float32)

    def add_both(d, c):
        @pl.when((z >= d) & needed(d, c))
        def _():
            add_down(z - d, c)

        @pl.when((z + d < lines) & needed(d, c))
        def _():
            add_down(z + d, c)

    def exchange(total, landing, ssem, rsem, c):
        return remote(total.at[c, theirs], landing.at[c], ssem.at[c], rsem.at[c], partner)

    def bring_home(total, landing, ssem, rsem, c):
        return remote(total.at[c, mine], landing.at[c], ssem.at[c], rsem.at[c], peer(c, half))

    def end_copy():
        target = jnp.where(z == 1, 0, lines - 1)
        return remote(acc2.at[0, mine], edge_in, esend.at[0], erecv.at[0], (target, e))

    loads[2].wait()
    loads[0].wait()
    loads[1].wait()
    loads[3].start()
    copies[0].wait_recv()
    make_hidden(0)
    send_own(0)
    start_lend(1)
    loads[3].wait()

    def chunk(c, carry):
        acc[c] = jnp.dot(hid[z, c], down_w[z], preferred_element_type=jnp.float32)
        pass_on(1, c)

        @pl.when(c == 0)
        def _():
            copies[1].wait_recv()
            copies[5].start()
            copies[3].start()
            copies[2].wait_recv()
            copies[6].start()
            copies[4].start()
            copies[5].wait_recv()

        @pl.when(c == 1)
        def _():
            copies[3].wait_recv()
            copies[4].wait_recv()
            copies[7].start()
            copies[6].wait_recv()

        @pl.when(c == 2)
        def _():
            copies[7].wait_recv()

        @pl.when(c < chunks - 1)
        def _():
            make_hidden(c + 1)

        if assist:

            @pl.when(helper & (c == last))
            def _():
                for k in range(chunks):
                    lend(k).wait_recv()
                for k in range(last):
                    acc2[k] = jnp.dot(
                        hid[far, k], far_w[...], preferred_element_type=jnp.float32
                    )
                    exchange(acc2, swap2, x2send, x2recv, k).start()
                for k in range(1, last):
                    exchange(acc2, swap2, x2send, x2recv, k).wait_recv()
                    acc2[k, mine] += swap2[k]
                    bring_home(acc2, ret2, r2send, r2recv, k).start()
                exchange(acc2, swap2, x2send, x2recv, 0).wait_recv()
                acc2[0, mine] = share[:, 0:1] * (acc2[0, mine] + swap2[0])

        for d in range(2, lines):
            pass_on(d, c)
            if d == 2:

                @pl.when(c < chunks - 1)
                def _():
                    send_own(c + 1)

                for k in range(2, chunks):

                    @pl.when(c == k - 2)
                    def _():
                        start_lend(k)

            add_both(d - 1, c)
        add_both(lines - 1, c)

        exchange(acc, swap, xsend, xrecv, c).start()
        exchange(acc, swap, xsend, xrecv, c).wait_recv()
        acc[c, mine] += swap[c]

        @pl.when(c > 0)
        def _():
            bring_home(acc, ret, rsend, rrecv, c).start()

        if assist:

            @pl.when(helper & (c == last))
            def _():
                for k in range(1, last):
                    bring_home(acc2, ret2, r2send, r2recv, k).wait_recv()
                    acc2[0, mine] += share[:, k : k + 1] * ret2[k]
                end_copy().start()

        return carry

    lax.fori_loop(0, chunks, chunk, 0)

    for j in range(lines):

        @pl.when(z != j)
        def _():
            remote(packed, states.at[j], ssend.at[j], srecv.at[j], (j, e)).wait_recv()

    gathered[...] = states[...]
    total = share[:, 0:1] * acc[0, mine]
    for c in range(1, chunks):
        bring_home(acc, ret, rsend, rrecv, c).wait_recv()
        total += share[:, c : c + 1] * ret[c]
    swap[0] = total
    if assist:

        @pl.when(edge)
        def _():
            end_copy().wait_recv()
            swap[0] += edge_in[...]

    out[...] = swap[0].astype(out.dtype)

    for j in range(lines):

        @pl.when(z != j)
        def _():
            state_copy(j).wait_send()

    if assist:

        @pl.when(edge)
        def _():
            for k in range(chunks):
                lend(k).wait_send()

        @pl.when(helper)
        def _():
            for k in range(last):
                exchange(acc2, swap2, x2send, x2recv, k).wait_send()
                if k > 0:
                    bring_home(acc2, ret2, r2send, r2recv, k).wait_send()
            end_copy().wait_send()

    for copy in copies:
        copy.wait_send()
    for c in range(chunks):
        for d in range(lines - 1):
            if assist and d == lines - 2 and c < last:
                continue

            @pl.when((z >= d) & (z < lines - 1))
            def _():
                to_right(d, c).wait_send()

            @pl.when((z + d < lines) & (z > 0))
            def _():
                to_left(d, c).wait_send()

        exchange(acc, swap, xsend, xrecv, c).wait_send()
        if c > 0:
            bring_home(acc, ret, rsend, rrecv, c).wait_send()


def expert_fused(packed, moe_tokens, expert_ids, route_weights, gate_proj, up_proj, down_proj):
    lines = lax.axis_size("ctx")
    chunks = GRID * GRID
    rows, width = moe_tokens.shape
    part = gate_proj.shape[2]
    columns = down_proj.shape[2]
    place = lax.axis_index("exp") // PAIR
    px, py = place % GRID, place // GRID
    order = jnp.stack(
        [((py + c // GRID) % GRID) * GRID + (px + c % GRID) % GRID for c in range(chunks)]
    )
    share = jnp.sum(
        jnp.where(expert_ids[:, :, None] == order[None, None, :], route_weights[:, :, None], 0.0),
        axis=1,
    )
    f32, bf16 = jnp.float32, jnp.bfloat16
    dma = pltpu.SemaphoreType.DMA
    vmem = pl.BlockSpec(memory_space=pltpu.VMEM)
    hbm = pl.BlockSpec(memory_space=pl.ANY)
    return pl.pallas_call(
        functools.partial(expert_kernel, lines),
        out_shape=(
            jax.ShapeDtypeStruct((rows, columns), bf16),
            jax.ShapeDtypeStruct((lines, *packed.shape), f32),
        ),
        in_specs=[vmem, vmem, vmem, hbm, hbm, hbm],
        out_specs=(vmem, vmem),
        scratch_shapes=[
            pltpu.VMEM((width, part), bf16),
            pltpu.VMEM((width, part), bf16),
            pltpu.VMEM((lines, part, columns), bf16),
            pltpu.VMEM((chunks, PAIR * rows, width), bf16),
            pltpu.VMEM((lines, chunks, PAIR * rows, part), bf16),
            pltpu.VMEM((chunks, PAIR * rows, columns), f32),
            pltpu.VMEM((chunks, rows, columns), f32),
            pltpu.VMEM((chunks, rows, columns), f32),
            pltpu.VMEM((part, columns), bf16),
            pltpu.VMEM((chunks - 1, PAIR * rows, columns), f32),
            pltpu.VMEM((chunks - 1, rows, columns), f32),
            pltpu.VMEM((chunks - 1, rows, columns), f32),
            pltpu.VMEM((rows, columns), f32),
            pltpu.VMEM((lines, *packed.shape), f32),
            dma((4,)),
            dma((8,)),
            dma((8,)),
            dma((lines, chunks)),
            dma((lines, chunks)),
            dma((lines, chunks)),
            dma((lines, chunks)),
            dma((chunks,)),
            dma((chunks,)),
            dma((chunks,)),
            dma((chunks,)),
            dma((lines,)),
            dma((lines,)),
            dma((chunks,)),
            dma((chunks,)),
            dma((chunks,)),
            dma((chunks,)),
            dma((chunks,)),
            dma((chunks,)),
            dma((1,)),
            dma((1,)),
        ],
        compiler_params=pltpu.CompilerParams(
            collective_id=0, has_side_effects=True, vmem_limit_bytes=VMEM_BYTES
        ),
    )(
        moe_tokens,
        share,
        packed,
        gate_proj[0],
        up_proj[0],
        down_proj[0].reshape(lines, part, columns),
    )


def expert_layer(packed, *arrays):
    moe_tokens, gate_proj, down_proj = arrays[0], arrays[3], arrays[5]
    if lax.axis_size("exp") == PAIR * GRID * GRID and gate_proj.shape[2] % 128 == 0:
        return expert_fused(packed, *arrays)
    return expert_block(*arrays), lax.all_gather(packed, "ctx")


def on_device(
    seq_inputs,
    step_size,
    write_map,
    read_map,
    decay_log,
    skip_gain,
    moe_tokens,
    expert_ids,
    route_weights,
    gate_proj,
    up_proj,
    down_proj,
):
    local_mix, cumulative, block_ends, entering, final = mixer_prepare(
        seq_inputs, step_size, write_map, read_map, decay_log
    )
    total_log = jnp.sum(block_ends, axis=1)
    head_count, state_count, head_width = final.shape
    logs = jnp.broadcast_to(total_log[:, None, None], (head_count, 8, head_width))
    packed = jnp.concatenate([final, logs], axis=1)
    expert_output, gathered = expert_layer(
        packed, moe_tokens, expert_ids, route_weights, gate_proj, up_proj, down_proj
    )
    place = lax.axis_index("ctx")
    state_before = jnp.zeros_like(final)
    for lap in range(lax.axis_size("ctx")):
        latter = gathered[lap]
        decay = jnp.exp(latter[:, state_count, 0])
        added = decay[:, None, None] * state_before + latter[:, :state_count]
        state_before = jnp.where(lap < place, added, state_before)
    mixer_output = mixer_finish(
        local_mix, cumulative, block_ends, entering, state_before, read_map, seq_inputs, skip_gain
    )
    return (mixer_output, expert_output)


def solution(mesh):
    return jax.shard_map(
        on_device,
        mesh=mesh,
        in_specs=(
            P("ctx", "exp"),
            P("exp", "ctx"),
            P(None, "ctx"),
            P(None, "ctx"),
            P("exp"),
            P("exp"),
            P("exp", None),
            P("exp", None),
            P("exp", None),
            P("exp", None, "ctx"),
            P("exp", None, "ctx"),
            P("exp", None, "ctx"),
        ),
        out_specs=(P("ctx", "exp"), P("exp", "ctx")),
        check_vma=False,
    )
```
